32 devices in a mesh: pts: 4 (over y, core), dir: 4 (over z), freq: 2 (over x).
Axes of the slice: x: 2, y: 2, z: 4, core: 2. Of those that a mesh axis runs over, the one named last changes fastest.
Arguments:
- action: float32 [48, 64, 16384], P('freq', 'dir', 'pts'), may hold values from 0.05 to 2
- bathymetry: float32 [16384], P('pts'), may hold values from 20 to 60
- refraction: float32 [48, 16384], P('freq', 'pts'), may hold values from 0.5 to 2
- shifting: float32 [48, 16384], P('freq', 'pts'), may hold values from 0.5 to 2
- heading: float32 [16384], P('pts'), may hold values from -3.140625 to 3.140625
- slope_angle: float32 [16384], P('pts'), may hold values from -3.140625 to 3.140625
- wet_mask: int32 [16384], P('pts'), may hold values 0 or 1
- substeps: int32 [32], P('pts'), may hold values from 1 to 4
Outputs:
- evolved: float32 [48, 64, 16384], P('freq', 'dir', 'pts')
The draws below stay inside these ranges and needn't reach their ends.
All inputs are finite; a program needn't handle non-finite values. Where the reference program divides by a largest or mean magnitude, that divisor is 1e-20 or more. No bound on the sum of `wet_mask` on one device may be relied on, other than what follows from the above.
Results may differ from the reference program's by a relative error of at most 0.00002.
Values sent between devices are 32-bit elements; how exact they have to be, the bound alone decides.
A program may use at most 64 MiB of HBM per device.

```python
import math
import jax
import jax.numpy as jnp
from jax import lax

FREQ = 48
DIR = 64
KMAX = 4
BLK = 512
P_DEV = 4096
PTS = 16384
NBLK = 32
N_PTS = 4


def place_ends(array, own_key, low, high):
    dims = array.shape
    spot = [jax.random.randint(jax.random.fold_in(own_key, axis), (), 0, dims[axis]) for axis in range(len(dims))]
    array = array.at[tuple(spot)].set(low)
    longest = dims.index(max(dims))
    spot[longest] = (spot[longest] + 1) % dims[longest]
    return array.at[tuple(spot)].set(high)


def block_scale(rng, dims, shards, least, high):
    def one(dim, parts):
        draws = jax.random.uniform(jax.random.fold_in(jax.random.fold_in(rng, 6), dim), (parts,), jnp.float32, least / len(shards), high / len(shards))
        return jnp.repeat(jnp.exp(draws), dims[dim] // parts).reshape((-1,) + (1,) * (len(dims) - dim - 1))

    gain = one(*shards[0])
    for cut in shards[1:]:
        gain = gain * one(*cut)
    return gain


def setup_inputs(seed: int = 0) -> dict:
    streams_of = jax.random.split(jax.random.key(seed), 9)
    action = jnp.clip(jnp.exp(math.log(2.0) - 3.6888794 * jax.random.uniform(streams_of[0], (FREQ, DIR, PTS), jnp.float32) ** block_scale(streams_of[0], (FREQ, DIR, PTS), ((0, 2), (1, 4), (2, 4)), -0.2, 0.2)), 0.05, 2.0)
    bathymetry = jnp.clip(20.0 + 40.0 * jax.random.uniform(streams_of[1], (PTS,), jnp.float32) ** block_scale(streams_of[1], (PTS,), ((0, 4),), -0.2, 0.2), 20.0, 60.0)
    refraction = jnp.clip(jnp.exp(math.log(2.0) - 1.3862944 * jax.random.uniform(streams_of[2], (FREQ, PTS), jnp.float32) ** block_scale(streams_of[2], (FREQ, PTS), ((0, 2), (1, 4)), -0.2, 0.2)), 0.5, 2.0)
    shifting = jnp.clip(jnp.exp(math.log(2.0) - 1.3862944 * jax.random.uniform(streams_of[3], (FREQ, PTS), jnp.float32) ** block_scale(streams_of[3], (FREQ, PTS), ((0, 2), (1, 4)), -0.2, 0.2)), 0.5, 2.0)
    heading = jnp.clip(jax.random.uniform(streams_of[4], (PTS,), jnp.float32, -3.140625, 3.140625), -3.140625, 3.140625)
    slope_angle = jnp.clip(jax.random.uniform(streams_of[5], (PTS,), jnp.float32, -3.140625, 3.140625), -3.140625, 3.140625)
    wet_mask = place_ends((jax.random.randint(streams_of[6], (PTS,), 0, 4) < 3).astype(jnp.int32), jax.random.fold_in(streams_of[6], 1), 0, 1)
    substeps = place_ends(jax.random.randint(streams_of[7], (NBLK,), 1, KMAX + 1), jax.random.fold_in(streams_of[7], 1), 1, KMAX).astype(jnp.int32)
    return dict(action=action, bathymetry=bathymetry, refraction=refraction, shifting=shifting, heading=heading, slope_angle=slope_angle, wet_mask=wet_mask, substeps=substeps)


EPSILON = 1e-6


def sweep(values, courant, weight, active, along):
    extent = values.shape[along]
    lower_cells = lax.slice_in_dim(values, 0, extent - 1, axis=along)
    upper_cells = lax.slice_in_dim(values, 1, extent, axis=along)
    interface = 0.5 * (lax.slice_in_dim(courant, 0, extent - 1, axis=along) + lax.slice_in_dim(courant, 1, extent, axis=along)) * weight
    fluxes = jnp.maximum(interface, 0.0) * lower_cells + jnp.minimum(interface, 0.0) * upper_cells
    change = lax.slice_in_dim(fluxes, 1, extent - 1, axis=along) - lax.slice_in_dim(fluxes, 0, extent - 2, axis=along)
    inner_cells = lax.slice_in_dim(values, 1, extent - 1, axis=along)
    return jnp.where(active, inner_cells - change, inner_cells)


def direction_angles(index):
    return (index.astype(jnp.float32) + 0.5) * (2.0 * math.pi / DIR)


def reference(action, bathymetry, refraction, shifting, heading, slope_angle, wet_mask, substeps):
    padded = jnp.concatenate([bathymetry[:1], bathymetry, bathymetry[-1:]])
    gradient = (padded[2:] - padded[:-2]) * 0.5
    wet_float = wet_mask.astype(jnp.float32)
    turn_base = refraction * gradient[None, :] * wet_float[None, :]
    shift_base = shifting * wet_float[None, :]
    angles = direction_angles(jnp.arange(DIR, dtype=jnp.int32))
    cos_peak = jnp.max(jnp.abs(jnp.cos(angles[:, None] - heading[None, :])), axis=0)
    sin_peak = jnp.max(jnp.abs(jnp.sin(angles[:, None] - slope_angle[None, :])), axis=0)
    peak_turn = jnp.max(jnp.abs(turn_base) * sin_peak[None, :])
    peak_shift = jnp.max(jnp.abs(shift_base) * cos_peak[None, :])
    scale_turn = 0.5 / (peak_turn + EPSILON)
    scale_shift = 0.5 / (peak_shift + EPSILON)
    point_counts = jnp.repeat(substeps, BLK)
    marks = jnp.arange(FREQ + 1, dtype=jnp.int32)
    freq_weight = jnp.where((marks >= 1) & (marks <= FREQ - 1), 1.0, 0.0).astype(jnp.float32)[:, None, None]

    def one_group(group_index, output):
        start = (group_index * P_DEV).astype(jnp.int32)
        spectrum = lax.dynamic_slice_in_dim(action, start, P_DEV, 2)
        turn_part = lax.dynamic_slice_in_dim(turn_base, start, P_DEV, 1)
        shift_part = lax.dynamic_slice_in_dim(shift_base, start, P_DEV, 1)
        heading_part = lax.dynamic_slice_in_dim(heading, start, P_DEV, 0)
        slope_part = lax.dynamic_slice_in_dim(slope_angle, start, P_DEV, 0)
        wet_part = lax.dynamic_slice_in_dim(wet_float, start, P_DEV, 0)
        count_part = lax.dynamic_slice_in_dim(point_counts, start, P_DEV, 0)
        count_float = count_part.astype(jnp.float32)
        sines = jnp.sin(angles[:, None] - slope_part[None, :])
        c_turn = turn_part[:, None, :] * sines[None, :, :]
        courant_turn = c_turn * scale_turn / count_float[None, None, :]
        courant_wrap = jnp.concatenate([courant_turn[:, -1:], courant_turn, courant_turn[:, :1]], axis=1)
        for sweep_index in range(KMAX):
            active = (sweep_index < count_part)[None, None, :]
            wrapped = jnp.concatenate([spectrum[:, -1:], spectrum, spectrum[:, :1]], axis=1)
            spectrum = sweep(wrapped, courant_wrap, 1.0, active, 1)
        cosines = jnp.cos(angles[:, None] - heading_part[None, :])
        c_shift = shift_part[:, None, :] * cosines[None, :, :]
        courant_shift = c_shift * scale_shift / count_float[None, None, :]
        courant_chain = jnp.pad(courant_shift, ((1, 1), (0, 0), (0, 0)))
        for sweep_index in range(KMAX):
            active = (sweep_index < count_part)[None, None, :]
            chained = jnp.pad(spectrum, ((1, 1), (0, 0), (0, 0)))
            spectrum = sweep(chained, courant_chain, freq_weight, active, 0)
        return lax.dynamic_update_slice_in_dim(output, spectrum * wet_part[None, None, :], start, 2)

    return lax.fori_loop(0, N_PTS, one_group, jnp.zeros_like(action))
```

```python
import functools
import math

import jax
import jax.numpy as jnp
from jax import lax
from jax.experimental import pallas as pl
from jax.experimental.pallas import tpu as pltpu
from jax.sharding import PartitionSpec as P

FREQ = 48
DIR = 64
KMAX = 4
BLK = 512
CHUNK = 256
LANES = 128
HALO = KMAX
SUB = 8
PIECES = 4

EPSILON = 1e-06
MESH = pl.DeviceIdType.MESH


def turn_row_of(f, part, own, halo, refraction, face, forward, active, rows, dir_local):
    spare = rows - dir_local - 2 * HALO
    if spare:
        cells = jnp.concatenate(
            [
                own[f, :, part],
                halo[f, :HALO, part],
                jnp.zeros((spare, face.shape[1]), jnp.float32),
                halo[f, HALO:, part],
            ],
            axis=0,
        )
    else:
        cells = jnp.concatenate([own[f, :, part], halo[f, :, part]], axis=0)
    rate = refraction[pl.ds(f, 1), part]
    for k in range(KMAX):
        flux = face * jnp.where(forward, cells, pltpu.roll(cells, rows - 1, 0))
        step = rate if k == 0 else rate * active[k]
        cells = cells - step * (flux - pltpu.roll(flux, 1, 0))
    return cells[:dir_local]


def shift_columns(part, ext, face_at, speed, wet, store, size):
    forward = speed > 0.0
    here, flux, out = [None] * KMAX, [None] * KMAX, [None] * KMAX

    def advance(t, k, there, skip_out=False):
        q = t - 2 * k
        beyond = face_at(k, q) * (speed * jnp.where(forward, here[k], there))
        cells = None if skip_out else here[k] - (beyond - flux[k])
        here[k], flux[k] = there, beyond
        return cells

    def ramp(t):
        before = list(out)
        for k in range(KMAX):
            q = t - 2 * k
            if q < k - 1 or q > size - 2 - k:
                continue
            there = ext[q + 1, :, part] if k == 0 else before[k - 1]
            if q == k - 1:
                here[k] = there
            elif q == k:
                advance(t, k, there, skip_out=True)
            else:
                out[k] = advance(t, k, there)
                if k == KMAX - 1:
                    store(q - HALO, out[k] * wet)

    here[0] = ext[0, :, part]
    first = 3 * (KMAX - 1) + 1
    last = size - 1
    for t in range(first):
        ramp(t)

    def step(t, carry):
        now_here, now_flux, now_out = carry
        here[:], flux[:] = list(now_here), list(now_flux)
        fresh = []
        for k in range(KMAX):
            there = ext[t + 1, :, part] if k == 0 else now_out[k - 1]
            fresh.append(advance(t, k, there))
        store(t - 2 * (KMAX - 1) - HALO, fresh[KMAX - 1] * wet)
        return tuple(here), tuple(flux), tuple(fresh[: KMAX - 1])

    trips = last - first
    unroll = 3 if trips % 3 == 0 else 1
    state = lax.fori_loop(first, last, step, (tuple(here), tuple(flux), tuple(out[: KMAX - 1])), unroll=unroll)
    here[:], flux[:], out[: KMAX - 1] = list(state[0]), list(state[1]), list(state[2])
    for t in range(last, size - KMAX + 2 * (KMAX - 1)):
        ramp(t)


def kernel(
    n_pts,
    n_dir,
    n_freq,
    action_ref,
    depth_hbm,
    refraction_hbm,
    shifting_hbm,
    heading_hbm,
    slope_hbm,
    wet_hbm,
    substeps_hbm,
    out_ref,
    tail_own,
    tail_halo,
    tail_ext,
    tail_refraction,
    tail_face,
    tail_speed,
    tail_steps,
    tail_rows,
    own,
    halo,
    ext,
    shext,
    face_shift,
    depth_ref,
    refraction_ref,
    shifting_ref,
    heading_ref,
    slope_ref,
    wet_ref,
    substeps_ref,
    turn_row,
    shift_row,
    count_row,
    trig,
    depth_in,
    peaks,
    own_sem,
    load_sem,
    edge_send,
    edge_recv,
    dir_send,
    dir_recv,
    freq_send,
    freq_recv,
    sh_send,
    sh_recv,
    depth_send,
    depth_recv,
    peak_send,
    peak_recv,
):
    freq_local, dir_local, points = own.shape
    chunks = points // CHUNK
    piece = points // PIECES
    rows = -(-(dir_local + 2 * HALO) // SUB) * SUB
    pts_at = lax.axis_index("pts")
    dir_at = lax.axis_index("dir")
    freq_at = lax.axis_index("freq")
    dir_up, dir_down = lax.rem(dir_at + 1, n_dir), lax.rem(dir_at + n_dir - 1, n_dir)
    pts_up, pts_down = lax.rem(pts_at + 1, n_pts), lax.rem(pts_at + n_pts - 1, n_pts)
    group = n_pts * n_freq
    member = pts_at * n_freq + freq_at
    has_above = freq_at < n_freq - 1
    has_below = freq_at > 0

    def peer(offset):
        other = lax.rem(member + offset, group)
        return {"pts": other // n_freq, "freq": lax.rem(other, n_freq)}

    barrier = pltpu.get_barrier_semaphore()
    for target in (dir_up, dir_down):
        pl.semaphore_signal(barrier, inc=1, device_id={"dir": target}, device_id_type=MESH)
    for offset in range(1, group):
        pl.semaphore_signal(barrier, inc=1, device_id=peer(offset), device_id_type=MESH)

    loads = [
        pltpu.make_async_copy(source, target, load_sem.at[i])
        for i, (source, target) in enumerate(
            (
                (slope_hbm, slope_ref),
                (heading_hbm, heading_ref),
                (depth_hbm, depth_ref),
                (wet_hbm, wet_ref),
                (refraction_hbm, refraction_ref),
                (shifting_hbm, shifting_ref),
                (substeps_hbm, substeps_ref),
            )
        )
    ]
    for copy in loads:
        copy.start()

    def own_copy(i):
        at = pl.ds(pl.multiple_of(i * piece, piece), piece)
        return pltpu.make_async_copy(action_ref.at[:, :, at], own.at[:, :, at], own_sem.at[i])

    for i in range(PIECES):
        own_copy(i).start()

    if n_freq == 1:
        edges = []
        inner, inner_size = 0, freq_local
    elif n_freq == 2:
        edges = [jnp.where(has_above, freq_local - HALO, 0)]
        inner, inner_size = jnp.where(has_above, 0, HALO), freq_local - HALO
    else:
        edges = [0, freq_local - HALO]
        inner, inner_size = HALO, freq_local - 2 * HALO

    def span(c):
        return pl.ds(pl.multiple_of(c * CHUNK, CHUNK), CHUNK)

    def piece_span(i):
        return pl.ds(pl.multiple_of(i * piece, piece), piece)

    def remote(src, dst, send, recv, where):
        return pltpu.make_async_remote_copy(
            src_ref=src, dst_ref=dst, send_sem=send, recv_sem=recv, device_id=where, device_id_type=MESH
        )

    def depth_copies():
        return (
            remote(
                depth_hbm.at[:, pl.ds(points - LANES, LANES)],
                depth_in.at[0],
                depth_send.at[0],
                depth_recv.at[0],
                {"pts": pts_up},
            ),
            remote(
                depth_hbm.at[:, pl.ds(0, LANES)],
                depth_in.at[1],
                depth_send.at[1],
                depth_recv.at[1],
                {"pts": pts_down},
            ),
        )

    def halo_copies(freqs, at, sends, recvs):
        return (
            remote(
                action_ref.at[freqs, pl.ds(dir_local - HALO, HALO), at],
                halo.at[freqs, pl.ds(HALO, HALO), at],
                sends[0],
                recvs[0],
                {"dir": dir_up},
            ),
            remote(
                action_ref.at[freqs, pl.ds(0, HALO), at],
                halo.at[freqs, pl.ds(0, HALO), at],
                sends[1],
                recvs[1],
                {"dir": dir_down},
            ),
        )

    def edge_copies(e, i):
        return halo_copies(
            pl.ds(edges[e], HALO),
            piece_span(i),
            [edge_send.at[way, e, i] for way in range(2)],
            [edge_recv.at[way, e, i] for way in range(2)],
        )

    def dir_copies(c):
        return halo_copies(
            pl.ds(inner, inner_size),
            span(c),
            [dir_send.at[way, c] for way in range(2)],
            [dir_recv.at[way, c] for way in range(2)],
        )

    above, below = lax.rem(freq_at + 1, n_freq), lax.rem(freq_at + n_freq - 1, n_freq)

    def rise(src, dst, send, recv):
        return remote(src, dst, send, recv, {"freq": above})

    def fall(src, dst, send, recv):
        return remote(src, dst, send, recv, {"freq": below})

    def freq_copies(i):
        at = piece_span(i)
        return (
            rise(
                ext.at[pl.ds(freq_local, HALO), :, at],
                ext.at[pl.ds(0, HALO), :, at],
                freq_send.at[0, i],
                freq_recv.at[0, i],
            ),
            fall(
                ext.at[pl.ds(HALO, HALO), :, at],
                ext.at[pl.ds(freq_local + HALO, HALO), :, at],
                freq_send.at[1, i],
                freq_recv.at[1, i],
            ),
        )

    def sh_copies():
        return (
            rise(
                shifting_hbm.at[pl.ds(freq_local - SUB, SUB)],
                shext.at[0],
                sh_send.at[0],
                sh_recv.at[0],
            ),
            fall(shifting_hbm.at[pl.ds(0, SUB)], shext.at[1], sh_send.at[1], sh_recv.at[1]),
        )

    def start_pair(pair):
        @pl.when(has_above)
        def _():
            pair[0].start()

        @pl.when(has_below)
        def _():
            pair[1].start()

    def wait_pair(pair):
        @pl.when(has_above)
        def _():
            pair[0].wait_send()
            pair[1].wait_recv()

        @pl.when(has_below)
        def _():
            pair[1].wait_send()
            pair[0].wait_recv()

    pl.semaphore_wait(barrier, 2 + group - 1)
    for copy in depth_copies():
        copy.start()
    for i in range(PIECES):
        for e in range(len(edges)):
            for copy in edge_copies(e, i):
                copy.start()

    @pl.loop(0, chunks)
    def _(c):
        for copy in dir_copies(c):
            copy.start()

    if n_freq > 1:
        start_pair(sh_copies())

    row = lax.broadcasted_iota(jnp.int32, (rows, CHUNK), 0)
    offset = jnp.where(row >= rows - HALO, row - rows, row)
    angle = ((dir_at * dir_local + offset).astype(jnp.float32) + 0.5) * (2.0 * math.pi / DIR)
    trig[0] = jnp.sin(angle)
    trig[1] = jnp.cos(angle)
    half = lax.broadcasted_iota(jnp.int32, (DIR // 2, LANES), 0)
    half_angle = (half.astype(jnp.float32) + 0.5) * (2.0 * math.pi / DIR)
    half_sin, half_cos = jnp.sin(half_angle), jnp.cos(half_angle)
    for copy in loads:
        copy.wait()
    wet = wet_ref[...].astype(jnp.float32)
    trig_row = (jnp.sin(slope_ref[...]), jnp.cos(slope_ref[...]), jnp.sin(heading_ref[...]), jnp.cos(heading_ref[...]))
    turn_row[1:2, :] = trig_row[0]
    turn_row[2:3, :] = trig_row[1]
    shift_row[1:2, :] = trig_row[2]
    shift_row[2:3, :] = trig_row[3]

    @pl.when(jnp.logical_not(has_below))
    def _():
        @pl.loop(0, HALO)
        def _(f):
            ext[f] = jnp.zeros((dir_local, points), jnp.float32)

    @pl.when(jnp.logical_not(has_above))
    def _():
        @pl.loop(freq_local + HALO, freq_local + 2 * HALO)
        def _(f):
            ext[f] = jnp.zeros((dir_local, points), jnp.float32)

    for copy in depth_copies():
        copy.wait()
    depth = depth_ref[...]
    lane = lax.broadcasted_iota(jnp.int32, (1, points), 1)
    before = jnp.where(pts_at == 0, depth[:, :1], depth_in[0][:, LANES - 1 :])
    after = jnp.where(pts_at == n_pts - 1, depth[:, points - 1 :], depth_in[1][:, :1])
    left = jnp.where(lane == 0, before, pltpu.roll(depth, 1, 1))
    right = jnp.where(lane == points - 1, after, pltpu.roll(depth, points - 1, 1))
    slope = (right - left) * 0.5 * wet
    turn_row[0:1, :] = slope
    shift_row[0:1, :] = wet

    def peak_step(i, carry):
        turn, shift = carry
        part = pl.ds(pl.multiple_of(i * LANES, LANES), LANES)
        sines = jnp.abs(half_sin * turn_row[2:3, part] - half_cos * turn_row[1:2, part])
        cosines = jnp.abs(half_cos * shift_row[2:3, part] + half_sin * shift_row[1:2, part])
        turn_peak = jnp.max(sines, axis=0, keepdims=True) * jnp.abs(turn_row[0:1, part])
        shift_peak = jnp.max(cosines, axis=0, keepdims=True) * shift_row[0:1, part]
        turn = jnp.maximum(turn, jnp.abs(refraction_ref[:, part]) * turn_peak)
        shift = jnp.maximum(shift, jnp.abs(shifting_ref[:, part]) * shift_peak)
        return turn, shift

    zero = jnp.zeros((freq_local, LANES), jnp.float32)
    turn, shift = lax.fori_loop(0, points // LANES, peak_step, (zero, zero))
    turn = jnp.max(jnp.max(turn, axis=0, keepdims=True), axis=1, keepdims=True)
    shift = jnp.max(jnp.max(shift, axis=0, keepdims=True), axis=1, keepdims=True)
    tile = lax.broadcasted_iota(jnp.int32, (SUB, LANES), 0)
    peaks[member] = jnp.where(tile < SUB // 2, turn, shift)

    def peak_copy(offset):
        return remote(
            peaks.at[member], peaks.at[member], peak_send.at[offset], peak_recv.at[offset], peer(offset)
        )

    def peak_arrival(offset):
        source = lax.rem(member + group - offset, group)
        return remote(
            peaks.at[source], peaks.at[source], peak_send.at[offset], peak_recv.at[offset], peer(offset)
        )

    for offset in range(1, group):
        peak_copy(offset).start()

    for block in range(points // BLK):
        part = pl.ds(block * BLK, BLK)
        count_row[0:1, part] = jnp.broadcast_to(
            substeps_ref[0:1, block : block + 1].astype(jnp.float32), (1, BLK)
        )
    count = count_row[0:1, :]
    for k in range(1, KMAX):
        count_row[k : k + 1, :] = jnp.where(count > k, 1.0, 0.0)

    if n_freq > 1:
        wait_pair(sh_copies())
    face_rows = freq_local + 2 * HALO
    first = freq_at * freq_local - HALO

    @pl.loop(0, points // CHUNK)
    def _(c):
        part = span(c)
        window = jnp.concatenate(
            [shext[0, :, part][SUB - HALO :], shifting_ref[:, part], shext[1, :, part][:HALO]], axis=0
        )
        following = jnp.concatenate([window[1:], window[:1]], axis=0)
        mark = first + lax.broadcasted_iota(jnp.int32, (face_rows, CHUNK), 0)
        valid = (mark >= 0) & (mark + 1 <= FREQ - 1)
        face = jnp.where(valid, 0.5 * (window + following), 0.0)
        face_shift[:face_rows, :, part] = face[:, None, :]
        for k in range(1, KMAX):
            face_shift[k * face_rows : (k + 1) * face_rows, :, part] = (face * count_row[k : k + 1, part])[:, None, :]

    for offset in range(1, group):
        peak_copy(offset).wait_send()
        peak_arrival(offset).wait_recv()
    top = jnp.max(peaks[...], axis=0)
    scale_turn = 0.5 / (top[0:1, 0:1] + EPSILON)
    scale_shift = 0.5 / (top[SUB // 2 : SUB // 2 + 1, 0:1] + EPSILON)
    turn_row[0:1, :] = turn_row[0:1, :] * scale_turn / count
    shift_row[3:4, :] = shift_row[0:1, :] * scale_shift / count

    def active_of(part):
        return [None] + [count_row[k : k + 1, part] for k in range(1, KMAX)]

    def turn_face(part):
        speed = (trig[0] * turn_row[2:3, part] - trig[1] * turn_row[1:2, part]) * turn_row[0:1, part]
        return 0.5 * (speed + pltpu.roll(speed, rows - 1, 0))

    def shift_speed(part):
        width = part.size
        return (
            trig[1, :dir_local, :width] * shift_row[2:3, part] + trig[0, :dir_local, :width] * shift_row[1:2, part]
        ) * shift_row[3:4, part]

    def turn_some(c, start, size):
        part = span(c)
        face = turn_face(part)
        forward = face > 0.0
        active = active_of(part)

        def one(f):
            ext[HALO + f, :, part] = turn_row_of(
                f, part, own, halo, refraction_ref, face, forward, active, rows, dir_local
            )

        @pl.loop(0, size // 2)
        def _(i):
            one(start + 2 * i)
            one(start + 2 * i + 1)

    def shift_chunk(c):
        @pl.loop(0, CHUNK // LANES)
        def _(h):
            part = pl.ds(pl.multiple_of(c * CHUNK + h * LANES, LANES), LANES)

            def store(f, value):
                out_ref[f, :, part] = value

            shift_columns(
                part,
                ext,
                lambda k, q: face_shift[k * face_rows + q, :, part],
                shift_speed(part),
                shift_row[0:1, part],
                store,
                face_rows,
            )

    per_piece = chunks // PIECES

    @pl.loop(0, PIECES)
    def _(i):
        own_copy(i).wait()
        for e in range(len(edges)):
            for copy in edge_copies(e, i):
                copy.wait()

        @pl.loop(0, per_piece)
        def _(c):
            for start in edges:
                turn_some(i * per_piece + c, start, HALO)

        if n_freq > 1:
            start_pair(freq_copies(i))

    @pl.loop(0, PIECES)
    def _(i):
        if n_freq > 1:
            wait_pair(freq_copies(i))

        @pl.loop(0, jnp.where(i == PIECES - 1, per_piece - 1, per_piece))
        def _(j):
            c = i * per_piece + j
            for copy in dir_copies(c):
                copy.wait()
            turn_some(c, inner, inner_size)
            shift_chunk(c)

    end = span(chunks - 1)
    tail_own[...] = own[:, :, end]
    tail_ext[...] = ext[:, :, end]
    tail_refraction[...] = refraction_ref[:, end]
    tail_face[...] = turn_face(end)
    tail_speed[...] = shift_speed(end)
    tail_steps[...] = face_shift[:, :, end]
    for k in range(1, KMAX):
        tail_rows[k : k + 1, :] = count_row[k : k + 1, end]
    tail_rows[0:1, :] = shift_row[0:1, end]
    for copy in dir_copies(chunks - 1):
        copy.wait()
    tail_halo[...] = halo[:, :, end]


def finish(
    n_freq,
    done,
    tail_own,
    tail_halo,
    tail_ext,
    tail_refraction,
    tail_face,
    tail_speed,
    tail_steps,
    tail_rows,
    out_hbm,
    ext,
    last,
    main_sem,
    last_sem,
):
    freq_local, dir_local, points = done.shape
    width = tail_own.shape[2]
    rows = tail_face.shape[0]
    pieces = main_sem.shape[0]
    each = freq_local // pieces
    head = points - width

    def main_copy(i):
        freqs = pl.ds(i * each, each)
        at = pl.ds(0, head)
        return pltpu.make_async_copy(done.at[freqs, :, at], out_hbm.at[freqs, :, at], main_sem.at[i])

    for i in range(pieces):
        main_copy(i).start()

    freq_at = lax.axis_index("freq")
    if n_freq == 1:
        inner, inner_size = 0, freq_local
    elif n_freq == 2:
        inner, inner_size = jnp.where(freq_at < n_freq - 1, 0, HALO), freq_local - HALO
    else:
        inner, inner_size = HALO, freq_local - 2 * HALO

    ext[...] = tail_ext[...]
    everything = pl.ds(0, width)
    face = tail_face[...]
    forward = face > 0.0
    active = [None] + [tail_rows[k : k + 1, :] for k in range(1, KMAX)]

    def one(f):
        ext[HALO + f] = turn_row_of(
            f, everything, tail_own, tail_halo, tail_refraction, face, forward, active, rows, dir_local
        )

    @pl.loop(0, inner_size // 2)
    def _(i):
        one(inner + 2 * i)
        one(inner + 2 * i + 1)

    @pl.loop(0, width // LANES)
    def _(h):
        part = pl.ds(pl.multiple_of(h * LANES, LANES), LANES)

        def store(f, value):
            last[f, :, part] = value

        shift_columns(
            part,
            ext,
            lambda k, q: tail_steps[k * (freq_local + 2 * HALO) + q, :, part],
            tail_speed[:, part],
            tail_rows[0:1, part],
            store,
            freq_local + 2 * HALO,
        )

    final = pltpu.make_async_copy(last, out_hbm.at[:, :, pl.ds(head, width)], last_sem)
    final.start()
    for i in range(pieces):
        main_copy(i).wait()
    final.wait()


def local(mesh, action, bathymetry, refraction, shifting, heading, slope_angle, wet_mask, substeps):
    freq_local, dir_local, points = action.shape
    n_pts, n_dir, n_freq = mesh.shape["pts"], mesh.shape["dir"], mesh.shape["freq"]
    chunks = points // CHUNK
    rows = -(-(dir_local + 2 * HALO) // SUB) * SUB
    face_rows = freq_local + 2 * HALO
    group = n_pts * n_freq
    vmem = pl.BlockSpec(memory_space=pltpu.VMEM)
    hbm = pl.BlockSpec(memory_space=pltpu.HBM)
    dma = pltpu.SemaphoreType.DMA
    f32 = jnp.float32
    n_edges = max(1, min(2, n_freq - 1))
    shapes = [
        (freq_local, dir_local, points),
        (freq_local, dir_local, CHUNK),
        (freq_local, 2 * HALO, CHUNK),
        (face_rows, dir_local, CHUNK),
        (freq_local, CHUNK),
        (rows, CHUNK),
        (dir_local, CHUNK),
        (KMAX * face_rows, 1, CHUNK),
        (SUB, CHUNK),
    ]
    parts = pl.pallas_call(
        functools.partial(kernel, n_pts, n_dir, n_freq),
        out_shape=[jax.ShapeDtypeStruct(shape, f32) for shape in shapes],
        in_specs=[hbm] * 8,
        out_specs=[vmem] * len(shapes),
        scratch_shapes=[
            pltpu.VMEM((freq_local, dir_local, points), f32),
            pltpu.VMEM((freq_local, 2 * HALO, points), f32),
            pltpu.VMEM((face_rows, dir_local, points), f32),
            pltpu.VMEM((2, SUB, points), f32),
            pltpu.VMEM((KMAX * face_rows, 1, points), f32),
            pltpu.VMEM((1, points), f32),
            pltpu.VMEM((freq_local, points), f32),
            pltpu.VMEM((freq_local, points), f32),
            pltpu.VMEM((1, points), f32),
            pltpu.VMEM((1, points), f32),
            pltpu.VMEM((1, points), jnp.int32),
            pltpu.VMEM((1, points // BLK), jnp.int32),
            pltpu.VMEM((SUB, points), f32),
            pltpu.VMEM((SUB, points), f32),
            pltpu.VMEM((SUB, points), f32),
            pltpu.VMEM((2, rows, CHUNK), f32),
            pltpu.VMEM((2, 1, LANES), f32),
            pltpu.VMEM((group, SUB, LANES), f32),
            dma((PIECES,)),
            dma((7,)),
            dma((2, n_edges, PIECES)),
            dma((2, n_edges, PIECES)),
            dma((2, chunks)),
            dma((2, chunks)),
            dma((2, PIECES)),
            dma((2, PIECES)),
            dma((2,)),
            dma((2,)),
            dma((2,)),
            dma((2,)),
            dma((group,)),
            dma((group,)),
        ],
        compiler_params=pltpu.CompilerParams(
            collective_id=0, has_side_effects=True, vmem_limit_bytes=44 * 1024 * 1024
        ),
    )(
        action,
        bathymetry.reshape(1, points),
        refraction,
        shifting,
        heading.reshape(1, points),
        slope_angle.reshape(1, points),
        wet_mask.reshape(1, points),
        substeps.reshape(1, -1),
    )
    return pl.pallas_call(
        functools.partial(finish, n_freq),
        out_shape=jax.ShapeDtypeStruct(action.shape, f32),
        in_specs=[vmem] * len(shapes),
        out_specs=hbm,
        scratch_shapes=[
            pltpu.VMEM((face_rows, dir_local, CHUNK), f32),
            pltpu.VMEM((freq_local, dir_local, CHUNK), f32),
            dma((6,)),
            dma(()),
        ],
        compiler_params=pltpu.CompilerParams(vmem_limit_bytes=8 * 1024 * 1024),
    )(*parts)


def solution(mesh):
    placed = (
        P("freq", "dir", "pts"),
        P("pts"),
        P("freq", "pts"),
        P("freq", "pts"),
        P("pts"),
        P("pts"),
        P("pts"),
        P("pts"),
    )
    return jax.shard_map(
        functools.partial(local, mesh),
        mesh=mesh,
        in_specs=placed,
        out_specs=P("freq", "dir", "pts"),
        check_vma=False,
    )
```

```python
import functools
import math

import jax
import jax.numpy as jnp
from jax import lax
from jax.experimental import pallas as pl
from jax.experimental.pallas import tpu as pltpu
from jax.sharding import PartitionSpec as P

FREQ = 48
DIR = 64
KMAX = 4
BLK = 512
CHUNK = 256
LANES = 128
HALO = KMAX
SUB = 8
PIECES = 4

EPSILON = 1e-06
MESH = pl.DeviceIdType.MESH


def turn_row_of(f, part, own, halo, refraction, face, forward, active, rows, dir_local):
    spare = rows - dir_local - 2 * HALO
    if spare:
        cells = jnp.concatenate(
            [
                own[f, :, part],
                halo[f, :HALO, part],
                jnp.zeros((spare, face.shape[1]), jnp.float32),
                halo[f, HALO:, part],
            ],
            axis=0,
        )
    else:
        cells = jnp.concatenate([own[f, :, part], halo[f, :, part]], axis=0)
    rate = refraction[pl.ds(f, 1), part]
    for k in range(KMAX):
        flux = face * jnp.where(forward, cells, pltpu.roll(cells, rows - 1, 0))
        step = rate if k == 0 else rate * active[k]
        cells = cells - step * (flux - pltpu.roll(flux, 1, 0))
    return cells[:dir_local]


def shift_columns(part, ext, face_at, speed, wet, store, size):
    forward = speed > 0.0
    here, flux, out = [None] * KMAX, [None] * KMAX, [None] * KMAX

    def advance(t, k, there, skip_out=False):
        q = t - 2 * k
        beyond = face_at(k, q) * (speed * jnp.where(forward, here[k], there))
        cells = None if skip_out else here[k] - (beyond - flux[k])
        here[k], flux[k] = there, beyond
        return cells

    def ramp(t):
        before = list(out)
        for k in range(KMAX):
            q = t - 2 * k
            if q < k - 1 or q > size - 2 - k:
                continue
            there = ext[q + 1, :, part] if k == 0 else before[k - 1]
            if q == k - 1:
                here[k] = there
            elif q == k:
                advance(t, k, there, skip_out=True)
            else:
                out[k] = advance(t, k, there)
                if k == KMAX - 1:
                    store(q - HALO, out[k] * wet)

    here[0] = ext[0, :, part]
    first = 3 * (KMAX - 1) + 1
    last = size - 1
    for t in range(first):
        ramp(t)

    def step(t, carry):
        now_here, now_flux, now_out = carry
        here[:], flux[:] = list(now_here), list(now_flux)
        fresh = []
        for k in range(KMAX):
            there = ext[t + 1, :, part] if k == 0 else now_out[k - 1]
            fresh.append(advance(t, k, there))
        store(t - 2 * (KMAX - 1) - HALO, fresh[KMAX - 1] * wet)
        return tuple(here), tuple(flux), tuple(fresh[: KMAX - 1])

    trips = last - first
    unroll = 3 if trips % 3 == 0 else 1
    state = lax.fori_loop(first, last, step, (tuple(here), tuple(flux), tuple(out[: KMAX - 1])), unroll=unroll)
    here[:], flux[:], out[: KMAX - 1] = list(state[0]), list(state[1]), list(state[2])
    for t in range(last, size - KMAX + 2 * (KMAX - 1)):
        ramp(t)


def kernel(
    n_pts,
    n_dir,
    n_freq,
    action_ref,
    depth_hbm,
    refraction_hbm,
    shifting_hbm,
    heading_hbm,
    slope_hbm,
    wet_hbm,
    substeps_hbm,
    out_ref,
    tail_own,
    tail_halo,
    tail_ext,
    tail_refraction,
    tail_face,
    tail_speed,
    tail_steps,
    tail_rows,
    own,
    halo,
    ext,
    shext,
    face_shift,
    depth_ref,
    refraction_ref,
    shifting_ref,
    heading_ref,
    slope_ref,
    wet_ref,
    substeps_ref,
    turn_row,
    shift_row,
    count_row,
    trig,
    depth_in,
    peaks,
    own_sem,
    load_sem,
    edge_send,
    edge_recv,
    dir_send,
    dir_recv,
    freq_send,
    freq_recv,
    sh_send,
    sh_recv,
    depth_send,
    depth_recv,
    peak_send,
    peak_recv,
):
    freq_local, dir_local, points = own.shape
    chunks = points // CHUNK
    piece = points // PIECES
    rows = -(-(dir_local + 2 * HALO) // SUB) * SUB
    pts_at = lax.axis_index("pts")
    dir_at = lax.axis_index("dir")
    freq_at = lax.axis_index("freq")
    dir_up, dir_down = lax.rem(dir_at + 1, n_dir), lax.rem(dir_at + n_dir - 1, n_dir)
    pts_up, pts_down = lax.rem(pts_at + 1, n_pts), lax.rem(pts_at + n_pts - 1, n_pts)
    group = n_pts * n_freq
    member = pts_at * n_freq + freq_at
    has_above = freq_at < n_freq - 1
    has_below = freq_at > 0

    def peer(offset):
        other = lax.rem(member + offset, group)
        return {"pts": other // n_freq, "freq": lax.rem(other, n_freq)}

    barrier = pltpu.get_barrier_semaphore()
    for target in (dir_up, dir_down):
        pl.semaphore_signal(barrier, inc=1, device_id={"dir": target}, device_id_type=MESH)
    for offset in range(1, group):
        pl.semaphore_signal(barrier, inc=1, device_id=peer(offset), device_id_type=MESH)

    loads = [
        pltpu.make_async_copy(source, target, load_sem.at[i])
        for i, (source, target) in enumerate(
            (
                (slope_hbm, slope_ref),
                (heading_hbm, heading_ref),
                (depth_hbm, depth_ref),
                (wet_hbm, wet_ref),
                (refraction_hbm, refraction_ref),
                (shifting_hbm, shifting_ref),
                (substeps_hbm, substeps_ref),
            )
        )
    ]
    for copy in loads:
        copy.start()

    def own_copy(i):
        at = pl.ds(pl.multiple_of(i * piece, piece), piece)
        return pltpu.make_async_copy(action_ref.at[:, :, at], own.at[:, :, at], own_sem.at[i])

    for i in range(PIECES):
        own_copy(i).start()

    if n_freq == 1:
        edges = []
        inner, inner_size = 0, freq_local
    elif n_freq == 2:
        edges = [jnp.where(has_above, freq_local - HALO, 0)]
        inner, inner_size = jnp.where(has_above, 0, HALO), freq_local - HALO
    else:
        edges = [0, freq_local - HALO]
        inner, inner_size = HALO, freq_local - 2 * HALO

    def span(c):
        return pl.ds(pl.multiple_of(c * CHUNK, CHUNK), CHUNK)

    def piece_span(i):
        return pl.ds(pl.multiple_of(i * piece, piece), piece)

    def remote(src, dst, send, recv, where):
        return pltpu.make_async_remote_copy(
            src_ref=src, dst_ref=dst, send_sem=send, recv_sem=recv, device_id=where, device_id_type=MESH
        )

    def depth_copies():
        return (
            remote(
                depth_hbm.at[:, pl.ds(points - LANES, LANES)],
                depth_in.at[0],
                depth_send.at[0],
                depth_recv.at[0],
                {"pts": pts_up},
            ),
            remote(
                depth_hbm.at[:, pl.ds(0, LANES)],
                depth_in.at[1],
                depth_send.at[1],
                depth_recv.at[1],
                {"pts": pts_down},
            ),
        )

    def halo_copies(freqs, at, sends, recvs):
        return (
            remote(
                action_ref.at[freqs, pl.ds(dir_local - HALO, HALO), at],
                halo.at[freqs, pl.ds(HALO, HALO), at],
                sends[0],
                recvs[0],
                {"dir": dir_up},
            ),
            remote(
                action_ref.at[freqs, pl.ds(0, HALO), at],
                halo.at[freqs, pl.ds(0, HALO), at],
                sends[1],
                recvs[1],
                {"dir": dir_down},
            ),
        )

    def edge_copies(e, i):
        return halo_copies(
            pl.ds(edges[e], HALO),
            piece_span(i),
            [edge_send.at[way, e, i] for way in range(2)],
            [edge_recv.at[way, e, i] for way in range(2)],
        )

    def dir_copies(c):
        return halo_copies(
            pl.ds(inner, inner_size),
            span(c),
            [dir_send.at[way, c] for way in range(2)],
            [dir_recv.at[way, c] for way in range(2)],
        )

    above, below = lax.rem(freq_at + 1, n_freq), lax.rem(freq_at + n_freq - 1, n_freq)

    def rise(src, dst, send, recv):
        return remote(src, dst, send, recv, {"freq": above})

    def fall(src, dst, send, recv):
        return remote(src, dst, send, recv, {"freq": below})

    def freq_copies(i):
        at = piece_span(i)
        return (
            rise(
                ext.at[pl.ds(freq_local, HALO), :, at],
                ext.at[pl.ds(0, HALO), :, at],
                freq_send.at[0, i],
                freq_recv.at[0, i],
            ),
            fall(
                ext.at[pl.ds(HALO, HALO), :, at],
                ext.at[pl.ds(freq_local + HALO, HALO), :, at],
                freq_send.at[1, i],
                freq_recv.at[1, i],
            ),
        )

    def sh_copies():
        return (
            rise(
                shifting_hbm.at[pl.ds(freq_local - SUB, SUB)],
                shext.at[0],
                sh_send.at[0],
                sh_recv.at[0],
            ),
            fall(shifting_hbm.at[pl.ds(0, SUB)], shext.at[1], sh_send.at[1], sh_recv.at[1]),
        )

    def start_pair(pair):
        @pl.when(has_above)
        def _():
            pair[0].start()

        @pl.when(has_below)
        def _():
            pair[1].start()

    def wait_pair(pair):
        @pl.when(has_above)
        def _():
            pair[0].wait_send()
            pair[1].wait_recv()

        @pl.when(has_below)
        def _():
            pair[1].wait_send()
            pair[0].wait_recv()

    pl.semaphore_wait(barrier, 2 + group - 1)
    for copy in depth_copies():
        copy.start()
    for i in range(PIECES):
        for e in range(len(edges)):
            for copy in edge_copies(e, i):
                copy.start()

    @pl.loop(0, chunks)
    def _(c):
        for copy in dir_copies(c):
            copy.start()

    if n_freq > 1:
        start_pair(sh_copies())

    row = lax.broadcasted_iota(jnp.int32, (rows, CHUNK), 0)
    offset = jnp.where(row >= rows - HALO, row - rows, row)
    angle = ((dir_at * dir_local + offset).astype(jnp.float32) + 0.5) * (2.0 * math.pi / DIR)
    trig[0] = jnp.sin(angle)
    trig[1] = jnp.cos(angle)
    half = lax.broadcasted_iota(jnp.int32, (DIR // 2, LANES), 0)
    half_angle = (half.astype(jnp.float32) + 0.5) * (2.0 * math.pi / DIR)
    half_sin, half_cos = jnp.sin(half_angle), jnp.cos(half_angle)
    for copy in loads:
        copy.wait()
    wet = wet_ref[...].astype(jnp.float32)
    trig_row = (jnp.sin(slope_ref[...]), jnp.cos(slope_ref[...]), jnp.sin(heading_ref[...]), jnp.cos(heading_ref[...]))
    turn_row[1:2, :] = trig_row[0]
    turn_row[2:3, :] = trig_row[1]
    shift_row[1:2, :] = trig_row[2]
    shift_row[2:3, :] = trig_row[3]

    @pl.when(jnp.logical_not(has_below))
    def _():
        @pl.loop(0, HALO)
        def _(f):
            ext[f] = jnp.zeros((dir_local, points), jnp.float32)

    @pl.when(jnp.logical_not(has_above))
    def _():
        @pl.loop(freq_local + HALO, freq_local + 2 * HALO)
        def _(f):
            ext[f] = jnp.zeros((dir_local, points), jnp.float32)

    for copy in depth_copies():
        copy.wait()
    depth = depth_ref[...]
    lane = lax.broadcasted_iota(jnp.int32, (1, points), 1)
    before = jnp.where(pts_at == 0, depth[:, :1], depth_in[0][:, LANES - 1 :])
    after = jnp.where(pts_at == n_pts - 1, depth[:, points - 1 :], depth_in[1][:, :1])
    left = jnp.where(lane == 0, before, pltpu.roll(depth, 1, 1))
    right = jnp.where(lane == points - 1, after, pltpu.roll(depth, points - 1, 1))
    slope = (right - left) * 0.5 * wet
    turn_row[0:1, :] = slope
    shift_row[0:1, :] = wet

    def peak_step(i, carry):
        turn, shift = carry
        part = pl.ds(pl.multiple_of(i * LANES, LANES), LANES)
        sines = jnp.abs(half_sin * turn_row[2:3, part] - half_cos * turn_row[1:2, part])
        cosines = jnp.abs(half_cos * shift_row[2:3, part] + half_sin * shift_row[1:2, part])
        turn_peak = jnp.max(sines, axis=0, keepdims=True) * jnp.abs(turn_row[0:1, part])
        shift_peak = jnp.max(cosines, axis=0, keepdims=True) * shift_row[0:1, part]
        turn = jnp.maximum(turn, jnp.abs(refraction_ref[:, part]) * turn_peak)
        shift = jnp.maximum(shift, jnp.abs(shifting_ref[:, part]) * shift_peak)
        return turn, shift

    zero = jnp.zeros((freq_local, LANES), jnp.float32)
    turn, shift = lax.fori_loop(0, points // LANES, peak_step, (zero, zero))
    turn = jnp.max(jnp.max(turn, axis=0, keepdims=True), axis=1, keepdims=True)
    shift = jnp.max(jnp.max(shift, axis=0, keepdims=True), axis=1, keepdims=True)
    tile = lax.broadcasted_iota(jnp.int32, (SUB, LANES), 0)
    peaks[member] = jnp.where(tile < SUB // 2, turn, shift)

    def peak_copy(offset):
        return remote(
            peaks.at[member], peaks.at[member], peak_send.at[offset], peak_recv.at[offset], peer(offset)
        )

    def peak_arrival(offset):
        source = lax.rem(member + group - offset, group)
        return remote(
            peaks.at[source], peaks.at[source], peak_send.at[offset], peak_recv.at[offset], peer(offset)
        )

    for offset in range(1, group):
        peak_copy(offset).start()

    for block in range(points // BLK):
        part = pl.ds(block * BLK, BLK)
        count_row[0:1, part] = jnp.broadcast_to(
            substeps_ref[0:1, block : block + 1].astype(jnp.float32), (1, BLK)
        )
    count = count_row[0:1, :]
    for k in range(1, KMAX):
        count_row[k : k + 1, :] = jnp.where(count > k, 1.0, 0.0)

    if n_freq > 1:
        wait_pair(sh_copies())
    face_rows = freq_local + 2 * HALO
    first = freq_at * freq_local - HALO

    @pl.loop(0, points // CHUNK)
    def _(c):
        part = span(c)
        window = jnp.concatenate(
            [shext[0, :, part][SUB - HALO :], shifting_ref[:, part], shext[1, :, part][:HALO]], axis=0
        )
        following = jnp.concatenate([window[1:], window[:1]], axis=0)
        mark = first + lax.broadcasted_iota(jnp.int32, (face_rows, CHUNK), 0)
        valid = (mark >= 0) & (mark + 1 <= FREQ - 1)
        face = jnp.where(valid, 0.5 * (window + following), 0.0)
        face_shift[:face_rows, :, part] = face[:, None, :]
        for k in range(1, KMAX):
            face_shift[k * face_rows : (k + 1) * face_rows, :, part] = (face * count_row[k : k + 1, part])[:, None, :]

    for offset in range(1, group):
        peak_copy(offset).wait_send()
        peak_arrival(offset).wait_recv()
    top = jnp.max(peaks[...], axis=0)
    scale_turn = 0.5 / (top[0:1, 0:1] + EPSILON)
    scale_shift = 0.5 / (top[SUB // 2 : SUB // 2 + 1, 0:1] + EPSILON)
    turn_row[0:1, :] = turn_row[0:1, :] * scale_turn / count
    shift_row[3:4, :] = shift_row[0:1, :] * scale_shift / count

    def active_of(part):
        return [None] + [count_row[k : k + 1, part] for k in range(1, KMAX)]

    def turn_face(part):
        speed = (trig[0] * turn_row[2:3, part] - trig[1] * turn_row[1:2, part]) * turn_row[0:1, part]
        return 0.5 * (speed + pltpu.roll(speed, rows - 1, 0))

    def shift_speed(part):
        width = part.size
        return (
            trig[1, :dir_local, :width] * shift_row[2:3, part] + trig[0, :dir_local, :width] * shift_row[1:2, part]
        ) * shift_row[3:4, part]

    def turn_some(c, start, size):
        part = span(c)
        face = turn_face(part)
        forward = face > 0.0
        active = active_of(part)

        def one(f):
            ext[HALO + f, :, part] = turn_row_of(
                f, part, own, halo, refraction_ref, face, forward, active, rows, dir_local
            )

        @pl.loop(0, size // 2)
        def _(i):
            one(start + 2 * i)
            one(start + 2 * i + 1)

    def shift_chunk(c):
        @pl.loop(0, CHUNK // LANES)
        def _(h):
            part = pl.ds(pl.multiple_of(c * CHUNK + h * LANES, LANES), LANES)

            def store(f, value):
                out_ref[f, :, part] = value

            shift_columns(
                part,
                ext,
                lambda k, q: face_shift[k * face_rows + q, :, part],
                shift_speed(part),
                shift_row[0:1, part],
                store,
                face_rows,
            )

    per_piece = chunks // PIECES

    @pl.loop(0, PIECES)
    def _(i):
        own_copy(i).wait()
        for e in range(len(edges)):
            for copy in edge_copies(e, i):
                copy.wait()

        @pl.loop(0, per_piece)
        def _(c):
            for start in edges:
                turn_some(i * per_piece + c, start, HALO)

        if n_freq > 1:
            start_pair(freq_copies(i))

    @pl.loop(0, PIECES)
    def _(i):
        if n_freq > 1:
            wait_pair(freq_copies(i))

        @pl.loop(0, jnp.where(i == PIECES - 1, per_piece - 1, per_piece))
        def _(j):
            c = i * per_piece + j
            for copy in dir_copies(c):
                copy.wait()
            turn_some(c, inner, inner_size)
            shift_chunk(c)

    end = span(chunks - 1)
    tail_own[...] = own[:, :, end]
    tail_ext[...] = ext[:, :, end]
    tail_refraction[...] = refraction_ref[:, end]
    tail_face[...] = turn_face(end)
    tail_speed[...] = shift_speed(end)
    tail_steps[...] = face_shift[:, :, end]
    for k in range(1, KMAX):
        tail_rows[k : k + 1, :] = count_row[k : k + 1, end]
    tail_rows[0:1, :] = shift_row[0:1, end]
    for copy in dir_copies(chunks - 1):
        copy.wait()
    tail_halo[...] = halo[:, :, end]


def finish(
    n_freq,
    done,
    tail_own,
    tail_halo,
    tail_ext,
    tail_refraction,
    tail_face,
    tail_speed,
    tail_steps,
    tail_rows,
    out_hbm,
    ext,
    last,
    main_sem,
    last_sem,
):
    freq_local, dir_local, points = done.shape
    width = tail_own.shape[2]
    rows = tail_face.shape[0]
    pieces = main_sem.shape[0]
    each = freq_local // pieces
    head = points - width

    def main_copy(i):
        freqs = pl.ds(i * each, each)
        at = pl.ds(0, head)
        return pltpu.make_async_copy(done.at[freqs, :, at], out_hbm.at[freqs, :, at], main_sem.at[i])

    for i in range(pieces):
        main_copy(i).start()

    freq_at = lax.axis_index("freq")
    if n_freq == 1:
        inner, inner_size = 0, freq_local
    elif n_freq == 2:
        inner, inner_size = jnp.where(freq_at < n_freq - 1, 0, HALO), freq_local - HALO
    else:
        inner, inner_size = HALO, freq_local - 2 * HALO

    ext[...] = tail_ext[...]
    everything = pl.ds(0, width)
    face = tail_face[...]
    forward = face > 0.0
    active = [None] + [tail_rows[k : k + 1, :] for k in range(1, KMAX)]

    def one(f):
        ext[HALO + f] = turn_row_of(
            f, everything, tail_own, tail_halo, tail_refraction, face, forward, active, rows, dir_local
        )

    @pl.loop(0, inner_size // 2)
    def _(i):
        one(inner + 2 * i)
        one(inner + 2 * i + 1)

    @pl.loop(0, width // LANES)
    def _(h):
        part = pl.ds(pl.multiple_of(h * LANES, LANES), LANES)

        def store(f, value):
            last[f, :, part] = value

        shift_columns(
            part,
            ext,
            lambda k, q: tail_steps[k * (freq_local + 2 * HALO) + q, :, part],
            tail_speed[:, part],
            tail_rows[0:1, part],
            store,
            freq_local + 2 * HALO,
        )

    final = pltpu.make_async_copy(last, out_hbm.at[:, :, pl.ds(head, width)], last_sem)
    final.start()
    for i in range(pieces):
        main_copy(i).wait()
    final.wait()


def local(mesh, action, bathymetry, refraction, shifting, heading, slope_angle, wet_mask, substeps):
    freq_local, dir_local, points = action.shape
    n_pts, n_dir, n_freq = mesh.shape["pts"], mesh.shape["dir"], mesh.shape["freq"]
    chunks = points // CHUNK
    rows = -(-(dir_local + 2 * HALO) // SUB) * SUB
    face_rows = freq_local + 2 * HALO
    group = n_pts * n_freq
    vmem = pl.BlockSpec(memory_space=pltpu.VMEM)
    hbm = pl.BlockSpec(memory_space=pltpu.HBM)
    dma = pltpu.SemaphoreType.DMA
    f32 = jnp.float32
    n_edges = max(1, min(2, n_freq - 1))
    shapes = [
        (freq_local, dir_local, points),
        (freq_local, dir_local, CHUNK),
        (freq_local, 2 * HALO, CHUNK),
        (face_rows, dir_local, CHUNK),
        (freq_local, CHUNK),
        (rows, CHUNK),
        (dir_local, CHUNK),
        (KMAX * face_rows, 1, CHUNK),
        (SUB, CHUNK),
    ]
    parts = pl.pallas_call(
        functools.partial(kernel, n_pts, n_dir, n_freq),
        out_shape=[jax.ShapeDtypeStruct(shape, f32) for shape in shapes],
        in_specs=[hbm] * 8,
        out_specs=[vmem] * len(shapes),
        scratch_shapes=[
            pltpu.VMEM((freq_local, dir_local, points), f32),
            pltpu.VMEM((freq_local, 2 * HALO, points), f32),
            pltpu.VMEM((face_rows, dir_local, points), f32),
            pltpu.VMEM((2, SUB, points), f32),
            pltpu.VMEM((KMAX * face_rows, 1, points), f32),
            pltpu.VMEM((1, points), f32),
            pltpu.VMEM((freq_local, points), f32),
            pltpu.VMEM((freq_local, points), f32),
            pltpu.VMEM((1, points), f32),
            pltpu.VMEM((1, points), f32),
            pltpu.VMEM((1, points), jnp.int32),
            pltpu.VMEM((1, points // BLK), jnp.int32),
            pltpu.VMEM((SUB, points), f32),
            pltpu.VMEM((SUB, points), f32),
            pltpu.VMEM((SUB, points), f32),
            pltpu.VMEM((2, rows, CHUNK), f32),
            pltpu.VMEM((2, 1, LANES), f32),
            pltpu.VMEM((group, SUB, LANES), f32),
            dma((PIECES,)),
            dma((7,)),
            dma((2, n_edges, PIECES)),
            dma((2, n_edges, PIECES)),
            dma((2, chunks)),
            dma((2, chunks)),
            dma((2, PIECES)),
            dma((2, PIECES)),
            dma((2,)),
            dma((2,)),
            dma((2,)),
            dma((2,)),
            dma((group,)),
            dma((group,)),
        ],
        compiler_params=pltpu.CompilerParams(
            collective_id=0, has_side_effects=True, vmem_limit_bytes=44 * 1024 * 1024
        ),
    )(
        *[
            pltpu.with_memory_space_constraint(array, pltpu.HBM)
            for array in (
                action,
                bathymetry.reshape(1, points),
                refraction,
                shifting,
                heading.reshape(1, points),
                slope_angle.reshape(1, points),
                wet_mask.reshape(1, points),
                substeps.reshape(1, -1),
            )
        ]
    )
    return pl.pallas_call(
        functools.partial(finish, n_freq),
        out_shape=jax.ShapeDtypeStruct(action.shape, f32),
        in_specs=[vmem] * len(shapes),
        out_specs=hbm,
        scratch_shapes=[
            pltpu.VMEM((face_rows, dir_local, CHUNK), f32),
            pltpu.VMEM((freq_local, dir_local, CHUNK), f32),
            dma((6,)),
            dma(()),
        ],
        compiler_params=pltpu.CompilerParams(vmem_limit_bytes=8 * 1024 * 1024),
    )(*parts)


def solution(mesh):
    placed = (
        P("freq", "dir", "pts"),
        P("pts"),
        P("freq", "pts"),
        P("freq", "pts"),
        P("pts"),
        P("pts"),
        P("pts"),
        P("pts"),
    )
    return jax.shard_map(
        functools.partial(local, mesh),
        mesh=mesh,
        in_specs=placed,
        out_specs=P("freq", "dir", "pts"),
        check_vma=False,
    )
```

```python
import functools
import math

import jax
import jax.numpy as jnp
from jax import lax
from jax.experimental import pallas as pl
from jax.experimental.pallas import tpu as pltpu
from jax.sharding import PartitionSpec as P

FREQ = 48
DIR = 64
KMAX = 4
BLK = 512
CHUNK = 256
LANES = 128
HALO = KMAX
SUB = 8
PIECES = 4
LEAD = 1

EPSILON = 1e-06
MESH = pl.DeviceIdType.MESH


def turn_row_of(f, part, own, halo, refraction, face, forward, active, rows, dir_local):
    spare = rows - dir_local - 2 * HALO
    if spare:
        cells = jnp.concatenate(
            [
                own[f, :, part],
                halo[f, :HALO, part],
                jnp.zeros((spare, face.shape[1]), jnp.float32),
                halo[f, HALO:, part],
            ],
            axis=0,
        )
    else:
        cells = jnp.concatenate([own[f, :, part], halo[f, :, part]], axis=0)
    rate = refraction[pl.ds(f, 1), part]
    for k in range(KMAX):
        flux = face * jnp.where(forward, cells, pltpu.roll(cells, rows - 1, 0))
        step = rate if k == 0 else rate * active[k]
        cells = cells - step * (flux - pltpu.roll(flux, 1, 0))
    return cells[:dir_local]


def shift_columns(part, ext, face_at, speed, wet, store, size):
    forward = speed > 0.0
    here, flux, out = [None] * KMAX, [None] * KMAX, [None] * KMAX

    def advance(t, k, there, skip_out=False):
        q = t - 2 * k
        beyond = face_at(k, q) * (speed * jnp.where(forward, here[k], there))
        cells = None if skip_out else here[k] - (beyond - flux[k])
        here[k], flux[k] = there, beyond
        return cells

    def ramp(t):
        before = list(out)
        for k in range(KMAX):
            q = t - 2 * k
            if q < k - 1 or q > size - 2 - k:
                continue
            there = ext[q + 1, :, part] if k == 0 else before[k - 1]
            if q == k - 1:
                here[k] = there
            elif q == k:
                advance(t, k, there, skip_out=True)
            else:
                out[k] = advance(t, k, there)
                if k == KMAX - 1:
                    store(q - HALO, out[k] * wet)

    here[0] = ext[0, :, part]
    first = 3 * (KMAX - 1) + 1
    last = size - 1
    for t in range(first):
        ramp(t)

    def step(t, carry):
        now_here, now_flux, now_out = carry
        here[:], flux[:] = list(now_here), list(now_flux)
        fresh = []
        for k in range(KMAX):
            there = ext[t + 1, :, part] if k == 0 else now_out[k - 1]
            fresh.append(advance(t, k, there))
        store(t - 2 * (KMAX - 1) - HALO, fresh[KMAX - 1] * wet)
        return tuple(here), tuple(flux), tuple(fresh[: KMAX - 1])

    trips = last - first
    unroll = 3 if trips % 3 == 0 else 1
    state = lax.fori_loop(first, last, step, (tuple(here), tuple(flux), tuple(out[: KMAX - 1])), unroll=unroll)
    here[:], flux[:], out[: KMAX - 1] = list(state[0]), list(state[1]), list(state[2])
    for t in range(last, size - KMAX + 2 * (KMAX - 1)):
        ramp(t)


def peak_stages(n_pts, n_freq):
    stages = []
    for axis, count in (("pts", n_pts), ("freq", n_freq)):
        if count & (count - 1) == 0:
            amount = 1
            while amount < count:
                stages.append([(axis, "swap", amount)])
                amount *= 2
        else:
            stages.append([(axis, "turn", amount) for amount in range(1, count)])
    return stages


def kernel(
    n_pts,
    n_dir,
    n_freq,
    action_ref,
    depth_hbm,
    refraction_hbm,
    shifting_hbm,
    heading_hbm,
    slope_hbm,
    wet_hbm,
    substeps_hbm,
    out_ref,
    tail_own,
    tail_halo,
    tail_ext,
    tail_refraction,
    tail_face,
    tail_speed,
    tail_steps,
    tail_rows,
    own,
    halo,
    ext,
    shext,
    face_shift,
    depth_ref,
    refraction_ref,
    shifting_ref,
    heading_ref,
    slope_ref,
    wet_ref,
    substeps_ref,
    turn_row,
    shift_row,
    count_row,
    trig,
    depth_in,
    peaks,
    own_sem,
    load_sem,
    edge_send,
    edge_recv,
    dir_send,
    dir_recv,
    freq_send,
    freq_recv,
    sh_send,
    sh_recv,
    depth_send,
    depth_recv,
    peak_send,
    peak_recv,
):
    freq_local, dir_local, points = own.shape
    chunks = points // CHUNK
    piece = points // PIECES
    rows = -(-(dir_local + 2 * HALO) // SUB) * SUB
    pts_at = lax.axis_index("pts")
    dir_at = lax.axis_index("dir")
    freq_at = lax.axis_index("freq")
    dir_up, dir_down = lax.rem(dir_at + 1, n_dir), lax.rem(dir_at + n_dir - 1, n_dir)
    has_above = freq_at < n_freq - 1
    has_below = freq_at > 0
    has_next = pts_at < n_pts - 1
    has_last = pts_at > 0
    stages = peak_stages(n_pts, n_freq)
    places = {"pts": (pts_at, n_pts), "freq": (freq_at, n_freq)}

    def partner(axis, kind, amount):
        at, count = places[axis]
        if kind == "swap":
            return {axis: at + amount * (1 - 2 * lax.rem(lax.div(at, amount), 2))}
        return {axis: lax.rem(at + amount, count)}

    barrier = pltpu.get_barrier_semaphore()

    def greet(where):
        pl.semaphore_signal(barrier, inc=1, device_id=where, device_id_type=MESH)

    neighbours = [(has_next, {"pts": pts_at + 1}), (has_last, {"pts": pts_at - 1})]
    if n_freq > 2:
        neighbours += [(has_above, {"freq": freq_at + 1}), (has_below, {"freq": freq_at - 1})]
    greet({"dir": dir_up})
    greet({"dir": dir_down})
    for stage in stages:
        for move in stage:
            greet(partner(*move))
    for there, where in neighbours:
        pl.when(there)(functools.partial(greet, where))

    def own_copy(i):
        at = pl.ds(pl.multiple_of(i * piece, piece), piece)
        return pltpu.make_async_copy(action_ref.at[:, :, at], own.at[:, :, at], own_sem.at[i])

    for i in range(PIECES):
        own_copy(i).start()

    loads = [
        pltpu.make_async_copy(source, target, load_sem.at[i])
        for i, (source, target) in enumerate(
            (
                (slope_hbm, slope_ref),
                (heading_hbm, heading_ref),
                (depth_hbm, depth_ref),
                (wet_hbm, wet_ref),
                (refraction_hbm, refraction_ref),
                (shifting_hbm, shifting_ref),
                (substeps_hbm, substeps_ref),
            )
        )
    ]
    for copy in loads:
        copy.start()

    if n_freq == 1:
        edges = []
        inner, inner_size = 0, freq_local
    elif n_freq == 2:
        edges = [jnp.where(has_above, freq_local - HALO, 0)]
        inner, inner_size = jnp.where(has_above, 0, HALO), freq_local - HALO
    else:
        edges = [0, freq_local - HALO]
        inner, inner_size = HALO, freq_local - 2 * HALO

    def span(c):
        return pl.ds(pl.multiple_of(c * CHUNK, CHUNK), CHUNK)

    def piece_span(i):
        return pl.ds(pl.multiple_of(i * piece, piece), piece)

    def remote(src, dst, send, recv, where):
        return pltpu.make_async_remote_copy(
            src_ref=src, dst_ref=dst, send_sem=send, recv_sem=recv, device_id=where, device_id_type=MESH
        )

    def depth_up():
        return remote(
            depth_hbm.at[:, pl.ds(points - LANES, LANES)],
            depth_in.at[0],
            depth_send.at[0],
            depth_recv.at[0],
            {"pts": pts_at + 1},
        )

    def depth_down():
        return remote(
            depth_hbm.at[:, pl.ds(0, LANES)],
            depth_in.at[1],
            depth_send.at[1],
            depth_recv.at[1],
            {"pts": pts_at - 1},
        )

    def halo_copy(way, freqs, at, send, recv):
        top = pl.ds(dir_local - HALO, HALO)
        source, target, where = (top, pl.ds(HALO, HALO), dir_up) if way == 0 else (
            pl.ds(0, HALO),
            pl.ds(0, HALO),
            dir_down,
        )
        return remote(own.at[freqs, source, at], halo.at[freqs, target, at], send, recv, {"dir": where})

    def edge_copy(way, e, i):
        return halo_copy(
            way, pl.ds(edges[e], HALO), piece_span(i), edge_send.at[way, e, i], edge_recv.at[way, e, i]
        )

    def dir_copy(way, c):
        return halo_copy(way, pl.ds(inner, inner_size), span(c), dir_send.at[way, c], dir_recv.at[way, c])

    above, below = lax.rem(freq_at + 1, n_freq), lax.rem(freq_at + n_freq - 1, n_freq)

    def rise(src, dst, send, recv):
        return remote(src, dst, send, recv, {"freq": above})

    def fall(src, dst, send, recv):
        return remote(src, dst, send, recv, {"freq": below})

    def freq_copies(i):
        at = piece_span(i)
        return (
            rise(
                ext.at[pl.ds(freq_local, HALO), :, at],
                ext.at[pl.ds(0, HALO), :, at],
                freq_send.at[0, i],
                freq_recv.at[0, i],
            ),
            fall(
                ext.at[pl.ds(HALO, HALO), :, at],
                ext.at[pl.ds(freq_local + HALO, HALO), :, at],
                freq_send.at[1, i],
                freq_recv.at[1, i],
            ),
        )

    def sh_copies():
        return (
            rise(
                shifting_hbm.at[pl.ds(freq_local - SUB, SUB)],
                shext.at[0],
                sh_send.at[0],
                sh_recv.at[0],
            ),
            fall(shifting_hbm.at[pl.ds(0, SUB)], shext.at[1], sh_send.at[1], sh_recv.at[1]),
        )

    def start_pair(pair):
        @pl.when(has_above)
        def _():
            pair[0].start()

        @pl.when(has_below)
        def _():
            pair[1].start()

    def wait_pair(pair):
        @pl.when(has_above)
        def _():
            pair[0].wait_send()
            pair[1].wait_recv()

        @pl.when(has_below)
        def _():
            pair[1].wait_send()
            pair[0].wait_recv()

    beside = jnp.minimum(pts_at, 1) + jnp.minimum(n_pts - 1 - pts_at, 1)
    if n_freq > 2:
        beside += jnp.minimum(freq_at, 1) + jnp.minimum(n_freq - 1 - freq_at, 1)
    pl.semaphore_wait(barrier, 2 + sum(len(stage) for stage in stages) + beside)

    @pl.when(has_next)
    def _():
        depth_up().start()

    @pl.when(has_last)
    def _():
        depth_down().start()

    def start_halos(far):
        ways = (0, 1) if far is None else (far, 1 - far)
        ahead = 0 if far is None else LEAD
        for i in range(PIECES):
            own_copy(i).wait()
            for e in range(len(edges)):
                for way in ways:
                    edge_copy(way, e, i).start()
        for c in range(ahead):
            dir_copy(ways[0], c).start()

        @pl.loop(0, chunks - ahead)
        def _(c):
            dir_copy(ways[0], c + ahead).start()
            dir_copy(ways[1], c).start()

        for c in range(chunks - ahead, chunks):
            dir_copy(ways[1], c).start()

    @pl.when(dir_at == 0)
    def _():
        start_halos(1)

    @pl.when(dir_at == n_dir - 1)
    def _():
        start_halos(0)

    @pl.when((dir_at > 0) & (dir_at < n_dir - 1))
    def _():
        start_halos(None)

    if n_freq > 1:
        start_pair(sh_copies())

    row = lax.broadcasted_iota(jnp.int32, (rows, CHUNK), 0)
    offset = jnp.where(row >= rows - HALO, row - rows, row)
    angle = ((dir_at * dir_local + offset).astype(jnp.float32) + 0.5) * (2.0 * math.pi / DIR)
    trig[0] = jnp.sin(angle)
    trig[1] = jnp.cos(angle)
    half = lax.broadcasted_iota(jnp.int32, (DIR // 2, LANES), 0)
    half_angle = (half.astype(jnp.float32) + 0.5) * (2.0 * math.pi / DIR)
    half_sin, half_cos = jnp.sin(half_angle), jnp.cos(half_angle)
    for copy in loads:
        copy.wait()
    wet = wet_ref[...].astype(jnp.float32)
    trig_row = (jnp.sin(slope_ref[...]), jnp.cos(slope_ref[...]), jnp.sin(heading_ref[...]), jnp.cos(heading_ref[...]))
    turn_row[1:2, :] = trig_row[0]
    turn_row[2:3, :] = trig_row[1]
    shift_row[1:2, :] = trig_row[2]
    shift_row[2:3, :] = trig_row[3]

    @pl.when(jnp.logical_not(has_below))
    def _():
        @pl.loop(0, HALO)
        def _(f):
            ext[f] = jnp.zeros((dir_local, points), jnp.float32)

    @pl.when(jnp.logical_not(has_above))
    def _():
        @pl.loop(freq_local + HALO, freq_local + 2 * HALO)
        def _(f):
            ext[f] = jnp.zeros((dir_local, points), jnp.float32)

    @pl.when(has_next)
    def _():
        depth_up().wait_send()
        depth_down().wait_recv()

    @pl.when(has_last)
    def _():
        depth_down().wait_send()
        depth_up().wait_recv()

    depth = depth_ref[...]
    lane = lax.broadcasted_iota(jnp.int32, (1, points), 1)
    before = jnp.where(pts_at == 0, depth[:, :1], depth_in[0][:, LANES - 1 :])
    after = jnp.where(pts_at == n_pts - 1, depth[:, points - 1 :], depth_in[1][:, :1])
    left = jnp.where(lane == 0, before, pltpu.roll(depth, 1, 1))
    right = jnp.where(lane == points - 1, after, pltpu.roll(depth, points - 1, 1))
    slope = (right - left) * 0.5 * wet
    turn_row[0:1, :] = slope
    shift_row[0:1, :] = wet

    def peak_step(i, carry):
        turn, shift = carry
        part = pl.ds(pl.multiple_of(i * LANES, LANES), LANES)
        sines = jnp.abs(half_sin * turn_row[2:3, part] - half_cos * turn_row[1:2, part])
        cosines = jnp.abs(half_cos * shift_row[2:3, part] + half_sin * shift_row[1:2, part])
        turn_peak = jnp.max(sines, axis=0, keepdims=True) * jnp.abs(turn_row[0:1, part])
        shift_peak = jnp.max(cosines, axis=0, keepdims=True) * shift_row[0:1, part]
        turn = jnp.maximum(turn, jnp.abs(refraction_ref[:, part]) * turn_peak)
        shift = jnp.maximum(shift, jnp.abs(shifting_ref[:, part]) * shift_peak)
        return turn, shift

    zero = jnp.zeros((freq_local, LANES), jnp.float32)
    turn, shift = lax.fori_loop(0, points // LANES, peak_step, (zero, zero))
    turn = jnp.max(jnp.max(turn, axis=0, keepdims=True), axis=1, keepdims=True)
    shift = jnp.max(jnp.max(shift, axis=0, keepdims=True), axis=1, keepdims=True)
    tile = lax.broadcasted_iota(jnp.int32, (SUB, LANES), 0)
    peaks[0] = jnp.where(tile < SUB // 2, turn, shift)

    def peak_copy(source, slot, move):
        return remote(
            peaks.at[source], peaks.at[slot], peak_send.at[slot], peak_recv.at[slot], partner(*move)
        )

    slots, taken = [], 1
    for stage in stages:
        slots.append((taken - 1, [(taken + i, move) for i, move in enumerate(stage)]))
        taken += len(stage) + 1
    for slot, move in slots[0][1] if slots else []:
        peak_copy(0, slot, move).start()

    for block in range(points // BLK):
        part = pl.ds(block * BLK, BLK)
        count_row[0:1, part] = jnp.broadcast_to(
            substeps_ref[0:1, block : block + 1].astype(jnp.float32), (1, BLK)
        )
    count = count_row[0:1, :]
    for k in range(1, KMAX):
        count_row[k : k + 1, :] = jnp.where(count > k, 1.0, 0.0)

    if n_freq > 1:
        wait_pair(sh_copies())
    face_rows = freq_local + 2 * HALO
    first = freq_at * freq_local - HALO

    @pl.loop(0, points // CHUNK)
    def _(c):
        part = span(c)
        window = jnp.concatenate(
            [shext[0, :, part][SUB - HALO :], shifting_ref[:, part], shext[1, :, part][:HALO]], axis=0
        )
        following = jnp.concatenate([window[1:], window[:1]], axis=0)
        mark = first + lax.broadcasted_iota(jnp.int32, (face_rows, CHUNK), 0)
        valid = (mark >= 0) & (mark + 1 <= FREQ - 1)
        face = jnp.where(valid, 0.5 * (window + following), 0.0)
        face_shift[:face_rows, :, part] = face[:, None, :]
        for k in range(1, KMAX):
            face_shift[k * face_rows : (k + 1) * face_rows, :, part] = (face * count_row[k : k + 1, part])[:, None, :]

    top = peaks[0]
    for at, (source, moves) in enumerate(slots):
        for slot, move in moves:
            if at:
                peak_copy(source, slot, move).start()
        for slot, move in moves:
            peak_copy(source, slot, move).wait()
            top = jnp.maximum(top, peaks[slot])
        if at + 1 < len(slots):
            peaks[slots[at + 1][0]] = top
    scale_turn = 0.5 / (top[0:1, 0:1] + EPSILON)
    scale_shift = 0.5 / (top[SUB // 2 : SUB // 2 + 1, 0:1] + EPSILON)
    turn_row[0:1, :] = turn_row[0:1, :] * scale_turn / count
    shift_row[3:4, :] = shift_row[0:1, :] * scale_shift / count

    def active_of(part):
        return [None] + [count_row[k : k + 1, part] for k in range(1, KMAX)]

    def turn_face(part):
        speed = (trig[0] * turn_row[2:3, part] - trig[1] * turn_row[1:2, part]) * turn_row[0:1, part]
        return 0.5 * (speed + pltpu.roll(speed, rows - 1, 0))

    def shift_speed(part):
        width = part.size
        return (
            trig[1, :dir_local, :width] * shift_row[2:3, part] + trig[0, :dir_local, :width] * shift_row[1:2, part]
        ) * shift_row[3:4, part]

    def turn_some(c, start, size):
        part = span(c)
        face = turn_face(part)
        forward = face > 0.0
        active = active_of(part)

        def one(f):
            ext[HALO + f, :, part] = turn_row_of(
                f, part, own, halo, refraction_ref, face, forward, active, rows, dir_local
            )

        @pl.loop(0, size // 2)
        def _(i):
            one(start + 2 * i)
            one(start + 2 * i + 1)

    def shift_chunk(c):
        @pl.loop(0, CHUNK // LANES)
        def _(h):
            part = pl.ds(pl.multiple_of(c * CHUNK + h * LANES, LANES), LANES)

            def store(f, value):
                out_ref[f, :, part] = value

            shift_columns(
                part,
                ext,
                lambda k, q: face_shift[k * face_rows + q, :, part],
                shift_speed(part),
                shift_row[0:1, part],
                store,
                face_rows,
            )

    per_piece = chunks // PIECES

    @pl.loop(0, PIECES)
    def _(i):
        for e in range(len(edges)):
            for way in range(2):
                edge_copy(way, e, i).wait()

        @pl.loop(0, per_piece)
        def _(c):
            for start in edges:
                turn_some(i * per_piece + c, start, HALO)

        if n_freq > 1:
            start_pair(freq_copies(i))

    @pl.loop(0, PIECES)
    def _(i):
        if n_freq > 1:
            wait_pair(freq_copies(i))

        @pl.loop(0, jnp.where(i == PIECES - 1, per_piece - 1, per_piece))
        def _(j):
            c = i * per_piece + j
            for way in range(2):
                dir_copy(way, c).wait()
            turn_some(c, inner, inner_size)
            shift_chunk(c)

    end = span(chunks - 1)
    tail_own[...] = own[:, :, end]
    tail_ext[...] = ext[:, :, end]
    tail_refraction[...] = refraction_ref[:, end]
    tail_face[...] = turn_face(end)
    tail_speed[...] = shift_speed(end)
    tail_steps[...] = face_shift[:, :, end]
    for k in range(1, KMAX):
        tail_rows[k : k + 1, :] = count_row[k : k + 1, end]
    tail_rows[0:1, :] = shift_row[0:1, end]
    for way in range(2):
        dir_copy(way, chunks - 1).wait()
    tail_halo[...] = halo[:, :, end]


def finish(
    n_freq,
    done,
    tail_own,
    tail_halo,
    tail_ext,
    tail_refraction,
    tail_face,
    tail_speed,
    tail_steps,
    tail_rows,
    out_hbm,
    ext,
    last,
    main_sem,
    last_sem,
):
    freq_local, dir_local, points = done.shape
    width = tail_own.shape[2]
    rows = tail_face.shape[0]
    pieces = main_sem.shape[0]
    each = freq_local // pieces
    head = points - width

    def main_copy(i):
        freqs = pl.ds(i * each, each)
        at = pl.ds(0, head)
        return pltpu.make_async_copy(done.at[freqs, :, at], out_hbm.at[freqs, :, at], main_sem.at[i])

    for i in range(pieces):
        main_copy(i).start()

    freq_at = lax.axis_index("freq")
    if n_freq == 1:
        inner, inner_size = 0, freq_local
    elif n_freq == 2:
        inner, inner_size = jnp.where(freq_at < n_freq - 1, 0, HALO), freq_local - HALO
    else:
        inner, inner_size = HALO, freq_local - 2 * HALO

    ext[...] = tail_ext[...]
    everything = pl.ds(0, width)
    face = tail_face[...]
    forward = face > 0.0
    active = [None] + [tail_rows[k : k + 1, :] for k in range(1, KMAX)]

    def one(f):
        ext[HALO + f] = turn_row_of(
            f, everything, tail_own, tail_halo, tail_refraction, face, forward, active, rows, dir_local
        )

    @pl.loop(0, inner_size // 2)
    def _(i):
        one(inner + 2 * i)
        one(inner + 2 * i + 1)

    @pl.loop(0, width // LANES)
    def _(h):
        part = pl.ds(pl.multiple_of(h * LANES, LANES), LANES)

        def store(f, value):
            last[f, :, part] = value

        shift_columns(
            part,
            ext,
            lambda k, q: tail_steps[k * (freq_local + 2 * HALO) + q, :, part],
            tail_speed[:, part],
            tail_rows[0:1, part],
            store,
            freq_local + 2 * HALO,
        )

    final = pltpu.make_async_copy(last, out_hbm.at[:, :, pl.ds(head, width)], last_sem)
    final.start()
    for i in range(pieces):
        main_copy(i).wait()
    final.wait()


def local(mesh, action, bathymetry, refraction, shifting, heading, slope_angle, wet_mask, substeps):
    freq_local, dir_local, points = action.shape
    n_pts, n_dir, n_freq = mesh.shape["pts"], mesh.shape["dir"], mesh.shape["freq"]
    chunks = points // CHUNK
    rows = -(-(dir_local + 2 * HALO) // SUB) * SUB
    face_rows = freq_local + 2 * HALO
    n_slots = 1 + sum(len(stage) + 1 for stage in peak_stages(n_pts, n_freq))
    vmem = pl.BlockSpec(memory_space=pltpu.VMEM)
    hbm = pl.BlockSpec(memory_space=pltpu.HBM)
    dma = pltpu.SemaphoreType.DMA
    f32 = jnp.float32
    n_edges = max(1, min(2, n_freq - 1))
    shapes = [
        (freq_local, dir_local, points),
        (freq_local, dir_local, CHUNK),
        (freq_local, 2 * HALO, CHUNK),
        (face_rows, dir_local, CHUNK),
        (freq_local, CHUNK),
        (rows, CHUNK),
        (dir_local, CHUNK),
        (KMAX * face_rows, 1, CHUNK),
        (SUB, CHUNK),
    ]
    parts = pl.pallas_call(
        functools.partial(kernel, n_pts, n_dir, n_freq),
        out_shape=[jax.ShapeDtypeStruct(shape, f32) for shape in shapes],
        in_specs=[hbm] * 8,
        out_specs=[vmem] * len(shapes),
        scratch_shapes=[
            pltpu.VMEM((freq_local, dir_local, points), f32),
            pltpu.VMEM((freq_local, 2 * HALO, points), f32),
            pltpu.VMEM((face_rows, dir_local, points), f32),
            pltpu.VMEM((2, SUB, points), f32),
            pltpu.VMEM((KMAX * face_rows, 1, points), f32),
            pltpu.VMEM((1, points), f32),
            pltpu.VMEM((freq_local, points), f32),
            pltpu.VMEM((freq_local, points), f32),
            pltpu.VMEM((1, points), f32),
            pltpu.VMEM((1, points), f32),
            pltpu.VMEM((1, points), jnp.int32),
            pltpu.VMEM((1, points // BLK), jnp.int32),
            pltpu.VMEM((SUB, points), f32),
            pltpu.VMEM((SUB, points), f32),
            pltpu.VMEM((SUB, points), f32),
            pltpu.VMEM((2, rows, CHUNK), f32),
            pltpu.VMEM((2, 1, LANES), f32),
            pltpu.VMEM((n_slots, SUB, LANES), f32),
            dma((PIECES,)),
            dma((7,)),
            dma((2, n_edges, PIECES)),
            dma((2, n_edges, PIECES)),
            dma((2, chunks)),
            dma((2, chunks)),
            dma((2, PIECES)),
            dma((2, PIECES)),
            dma((2,)),
            dma((2,)),
            dma((2,)),
            dma((2,)),
            dma((n_slots,)),
            dma((n_slots,)),
        ],
        compiler_params=pltpu.CompilerParams(
            collective_id=0, has_side_effects=True, vmem_limit_bytes=44 * 1024 * 1024
        ),
    )(
        *[
            pltpu.with_memory_space_constraint(array, pltpu.HBM)
            for array in (
                action,
                bathymetry.reshape(1, points),
                refraction,
                shifting,
                heading.reshape(1, points),
                slope_angle.reshape(1, points),
                wet_mask.reshape(1, points),
                substeps.reshape(1, -1),
            )
        ]
    )
    return pl.pallas_call(
        functools.partial(finish, n_freq),
        out_shape=jax.ShapeDtypeStruct(action.shape, f32),
        in_specs=[vmem] * len(shapes),
        out_specs=hbm,
        scratch_shapes=[
            pltpu.VMEM((face_rows, dir_local, CHUNK), f32),
            pltpu.VMEM((freq_local, dir_local, CHUNK), f32),
            dma((6,)),
            dma(()),
        ],
        compiler_params=pltpu.CompilerParams(vmem_limit_bytes=8 * 1024 * 1024),
    )(*parts)


def solution(mesh):
    placed = (
        P("freq", "dir", "pts"),
        P("pts"),
        P("freq", "pts"),
        P("freq", "pts"),
        P("pts"),
        P("pts"),
        P("pts"),
        P("pts"),
    )
    return jax.shard_map(
        functools.partial(local, mesh),
        mesh=mesh,
        in_specs=placed,
        out_specs=P("freq", "dir", "pts"),
        check_vma=False,
    )
```

```python
import functools
import math

import jax
import jax.numpy as jnp
from jax import lax
from jax.experimental import pallas as pl
from jax.experimental.pallas import tpu as pltpu
from jax.sharding import PartitionSpec as P

FREQ = 48
DIR = 64
KMAX = 4
BLK = 512
CHUNK = 256
LANES = 128
HALO = KMAX
SUB = 8
PIECES = 4
LEAD = 1

EPSILON = 1e-06
MESH = pl.DeviceIdType.MESH


def turn_row_of(f, part, own, halo, refraction, face, forward, active, rows, dir_local):
    spare = rows - dir_local - 2 * HALO
    if spare:
        cells = jnp.concatenate(
            [
                own[f, :, part],
                halo[f, :HALO, part],
                jnp.zeros((spare, face.shape[1]), jnp.float32),
                halo[f, HALO:, part],
            ],
            axis=0,
        )
    else:
        cells = jnp.concatenate([own[f, :, part], halo[f, :, part]], axis=0)
    rate = refraction[pl.ds(f, 1), part]
    for k in range(KMAX):
        flux = face * jnp.where(forward, cells, pltpu.roll(cells, rows - 1, 0))
        step = rate if k == 0 else rate * active[k]
        cells = cells - step * (flux - pltpu.roll(flux, 1, 0))
    return cells[:dir_local]


def shift_columns(part, ext, face_at, speed, wet, store, size):
    forward = speed > 0.0
    here, flux, out = [None] * KMAX, [None] * KMAX, [None] * KMAX

    def advance(t, k, there, skip_out=False):
        q = t - 2 * k
        beyond = face_at(k, q) * (speed * jnp.where(forward, here[k], there))
        cells = None if skip_out else here[k] - (beyond - flux[k])
        here[k], flux[k] = there, beyond
        return cells

    def ramp(t):
        before = list(out)
        for k in range(KMAX):
            q = t - 2 * k
            if q < k - 1 or q > size - 2 - k:
                continue
            there = ext[q + 1, :, part] if k == 0 else before[k - 1]
            if q == k - 1:
                here[k] = there
            elif q == k:
                advance(t, k, there, skip_out=True)
            else:
                out[k] = advance(t, k, there)
                if k == KMAX - 1:
                    store(q - HALO, out[k] * wet)

    here[0] = ext[0, :, part]
    first = 3 * (KMAX - 1) + 1
    last = size - 1
    for t in range(first):
        ramp(t)

    def step(t, carry):
        now_here, now_flux, now_out = carry
        here[:], flux[:] = list(now_here), list(now_flux)
        fresh = []
        for k in range(KMAX):
            there = ext[t + 1, :, part] if k == 0 else now_out[k - 1]
            fresh.append(advance(t, k, there))
        store(t - 2 * (KMAX - 1) - HALO, fresh[KMAX - 1] * wet)
        return tuple(here), tuple(flux), tuple(fresh[: KMAX - 1])

    trips = last - first
    unroll = 3 if trips % 3 == 0 else 1
    state = lax.fori_loop(first, last, step, (tuple(here), tuple(flux), tuple(out[: KMAX - 1])), unroll=unroll)
    here[:], flux[:], out[: KMAX - 1] = list(state[0]), list(state[1]), list(state[2])
    for t in range(last, size - KMAX + 2 * (KMAX - 1)):
        ramp(t)


def peak_stages(n_pts, n_freq):
    stages = []
    for axis, count in (("pts", n_pts), ("freq", n_freq)):
        if count & (count - 1) == 0:
            amount = 1
            while amount < count:
                stages.append([(axis, "swap", amount)])
                amount *= 2
        else:
            stages.append([(axis, "turn", amount) for amount in range(1, count)])
    return stages


def kernel(
    n_pts,
    n_dir,
    n_freq,
    action_ref,
    depth_hbm,
    refraction_hbm,
    shifting_hbm,
    heading_hbm,
    slope_hbm,
    wet_hbm,
    substeps_hbm,
    out_ref,
    tail_own,
    tail_halo,
    tail_ext,
    tail_refraction,
    tail_face,
    tail_speed,
    tail_steps,
    tail_rows,
    own,
    halo,
    ext,
    shext,
    face_shift,
    depth_ref,
    refraction_ref,
    shifting_ref,
    heading_ref,
    slope_ref,
    wet_ref,
    substeps_ref,
    turn_row,
    shift_row,
    count_row,
    trig,
    depth_in,
    peaks,
    own_sem,
    own_edge_sem,
    load_sem,
    edge_send,
    edge_recv,
    dir_send,
    dir_recv,
    freq_send,
    freq_recv,
    sh_send,
    sh_recv,
    depth_send,
    depth_recv,
    peak_send,
    peak_recv,
    dir_ready,
    stage_ready,
    next_ready,
):
    freq_local, dir_local, points = own.shape
    chunks = points // CHUNK
    piece = points // PIECES
    rows = -(-(dir_local + 2 * HALO) // SUB) * SUB
    pts_at = lax.axis_index("pts")
    dir_at = lax.axis_index("dir")
    freq_at = lax.axis_index("freq")
    dir_up, dir_down = lax.rem(dir_at + 1, n_dir), lax.rem(dir_at + n_dir - 1, n_dir)
    has_above = freq_at < n_freq - 1
    has_below = freq_at > 0
    has_next = pts_at < n_pts - 1
    has_last = pts_at > 0
    stages = peak_stages(n_pts, n_freq)
    places = {"pts": (pts_at, n_pts), "freq": (freq_at, n_freq)}

    def partner(axis, kind, amount):
        at, count = places[axis]
        if kind == "swap":
            return {axis: at + amount * (1 - 2 * lax.rem(lax.div(at, amount), 2))}
        return {axis: lax.rem(at + amount, count)}

    def bit(axis, amount):
        return lax.rem(lax.div(places[axis][0], amount), 2)

    neighbours = [(0, has_next, has_last, "pts")]
    if n_freq > 2:
        neighbours.append((1, has_above, has_below, "freq"))
    barrier = pltpu.get_barrier_semaphore()

    def greet(where):
        pl.semaphore_signal(barrier, inc=1, device_id=where, device_id_type=MESH)

    last_dir = n_dir - 1

    @pl.when(dir_at < last_dir)
    def _():
        greet({"dir": dir_up})

    @pl.when(dir_at == 1)
    def _():
        greet({"dir": dir_down})

    @pl.when(dir_at == 0)
    def _():
        greet({"dir": dir_down})

    parents = 1 + lax.div(dir_at, last_dir)
    for stage in stages:
        for axis, kind, amount in stage:
            if kind == "swap":
                pl.when(bit(axis, amount) == 0)(functools.partial(greet, partner(axis, kind, amount)))
                parents += bit(axis, amount)
            else:
                greet(partner(axis, kind, amount))
                parents += 1
    for _, up_there, _, axis in neighbours:
        pl.when(up_there)(functools.partial(greet, {axis: places[axis][0] + 1}))
        parents += jnp.minimum(places[axis][0], 1)

    if n_freq == 1:
        edges = []
        inner, inner_size = 0, freq_local
    elif n_freq == 2:
        edges = [jnp.where(has_above, freq_local - HALO, 0)]
        inner, inner_size = jnp.where(has_above, 0, HALO), freq_local - HALO
    else:
        edges = [0, freq_local - HALO]
        inner, inner_size = HALO, freq_local - 2 * HALO

    def span(c):
        return pl.ds(pl.multiple_of(c * CHUNK, CHUNK), CHUNK)

    def piece_span(i):
        return pl.ds(pl.multiple_of(i * piece, piece), piece)

    def own_part(freqs, i, sem):
        at = piece_span(i)
        return pltpu.make_async_copy(action_ref.at[freqs, :, at], own.at[freqs, :, at], sem)

    def own_edge(e, i):
        return own_part(pl.ds(edges[e], HALO), i, own_edge_sem.at[e, i])

    def own_inner(i):
        return own_part(pl.ds(inner, inner_size), i, own_sem.at[i])

    for i in range(PIECES):
        for e in range(len(edges)):
            own_edge(e, i).start()
    for i in range(PIECES):
        own_inner(i).start()

    loads = [
        pltpu.make_async_copy(source, target, load_sem.at[i])
        for i, (source, target) in enumerate(
            (
                (slope_hbm, slope_ref),
                (heading_hbm, heading_ref),
                (depth_hbm, depth_ref),
                (wet_hbm, wet_ref),
                (refraction_hbm, refraction_ref),
                (shifting_hbm, shifting_ref),
                (substeps_hbm, substeps_ref),
            )
        )
    ]
    for copy in loads:
        copy.start()

    def remote(src, dst, send, recv, where):
        return pltpu.make_async_remote_copy(
            src_ref=src, dst_ref=dst, send_sem=send, recv_sem=recv, device_id=where, device_id_type=MESH
        )

    def depth_up():
        return remote(
            depth_hbm.at[:, pl.ds(points - LANES, LANES)],
            depth_in.at[0],
            depth_send.at[0],
            depth_recv.at[0],
            {"pts": pts_at + 1},
        )

    def depth_down():
        return remote(
            depth_hbm.at[:, pl.ds(0, LANES)],
            depth_in.at[1],
            depth_send.at[1],
            depth_recv.at[1],
            {"pts": pts_at - 1},
        )

    def halo_copy(way, freqs, at, send, recv):
        top = pl.ds(dir_local - HALO, HALO)
        source, target, where = (top, pl.ds(HALO, HALO), dir_up) if way == 0 else (
            pl.ds(0, HALO),
            pl.ds(0, HALO),
            dir_down,
        )
        return remote(own.at[freqs, source, at], halo.at[freqs, target, at], send, recv, {"dir": where})

    def edge_copy(way, e, i):
        return halo_copy(
            way, pl.ds(edges[e], HALO), piece_span(i), edge_send.at[way, e, i], edge_recv.at[way, e, i]
        )

    def dir_copy(way, c):
        return halo_copy(way, pl.ds(inner, inner_size), span(c), dir_send.at[way, c], dir_recv.at[way, c])

    above, below = lax.rem(freq_at + 1, n_freq), lax.rem(freq_at + n_freq - 1, n_freq)

    def rise(src, dst, send, recv):
        return remote(src, dst, send, recv, {"freq": above})

    def fall(src, dst, send, recv):
        return remote(src, dst, send, recv, {"freq": below})

    def freq_copies(i):
        at = piece_span(i)
        return (
            rise(
                ext.at[pl.ds(freq_local, HALO), :, at],
                ext.at[pl.ds(0, HALO), :, at],
                freq_send.at[0, i],
                freq_recv.at[0, i],
            ),
            fall(
                ext.at[pl.ds(HALO, HALO), :, at],
                ext.at[pl.ds(freq_local + HALO, HALO), :, at],
                freq_send.at[1, i],
                freq_recv.at[1, i],
            ),
        )

    def sh_copies():
        return (
            rise(
                shifting_hbm.at[pl.ds(freq_local - SUB, SUB)],
                shext.at[0],
                sh_send.at[0],
                sh_recv.at[0],
            ),
            fall(shifting_hbm.at[pl.ds(0, SUB)], shext.at[1], sh_send.at[1], sh_recv.at[1]),
        )

    def start_pair(pair):
        @pl.when(has_above)
        def _():
            pair[0].start()

        @pl.when(has_below)
        def _():
            pair[1].start()

    def wait_pair(pair):
        @pl.when(has_above)
        def _():
            pair[0].wait_send()
            pair[1].wait_recv()

        @pl.when(has_below)
        def _():
            pair[1].wait_send()
            pair[0].wait_recv()

    def report(sem, where):
        pl.semaphore_signal(sem, inc=1, device_id=where, device_id_type=MESH)

    pl.semaphore_wait(barrier, parents)

    @pl.when(dir_at > 1)
    def _():
        report(dir_ready, {"dir": dir_down})

    @pl.when(dir_at == last_dir)
    def _():
        report(dir_ready, {"dir": dir_up})

    for at, stage in enumerate(stages):
        for axis, kind, amount in stage:
            if kind == "swap":
                below_there = bit(axis, amount) == 1
                pl.when(below_there)(functools.partial(report, stage_ready.at[at], partner(axis, kind, amount)))
    for i, up_there, down_there, axis in neighbours:
        pl.when(down_there)(functools.partial(report, next_ready.at[i], {axis: places[axis][0] - 1}))
    def start_edges(way, low=0, high=PIECES):
        for i in range(low, high):
            for e in range(len(edges)):
                edge_copy(way, e, i).start()

    def start_inner(first, ahead):
        for c in range(ahead):
            dir_copy(first, c).start()

        @pl.loop(0, chunks - ahead)
        def _(c):
            dir_copy(first, c + ahead).start()
            dir_copy(1 - first, c).start()

        for c in range(chunks - ahead, chunks):
            dir_copy(1 - first, c).start()

    for i in range(PIECES):
        for e in range(len(edges)):
            own_edge(e, i).wait()

    is_end = (dir_at == 0) | (dir_at == last_dir)

    @pl.when(dir_at == 0)
    def _():
        start_edges(0, 0, 1)

    @pl.when(dir_at == last_dir)
    def _():
        start_edges(0, 0, 1)

    @pl.when(jnp.logical_not(is_end))
    def _():
        start_edges(1)


    @pl.when(dir_at < last_dir)
    def _():
        pl.semaphore_wait(dir_ready, 1)

    for i in range(PIECES):
        own_inner(i).wait()

    @pl.when(dir_at == 0)
    def _():
        for i in range(PIECES):
            start_edges(1, i, i + 1)
            if i + 1 < PIECES:
                start_edges(0, i + 1, i + 2)
        start_inner(1, LEAD)

    @pl.when(dir_at == last_dir)
    def _():
        for i in range(PIECES):
            start_edges(1, i, i + 1)
            if i + 1 < PIECES:
                start_edges(0, i + 1, i + 2)
        start_inner(0, LEAD)

    @pl.when(jnp.logical_not(is_end))
    def _():
        start_edges(0)
        start_inner(0, 0)

    for at, stage in enumerate(stages):
        for axis, kind, amount in stage:
            if kind == "swap":

                @pl.when(bit(axis, amount) == 0)
                def _():
                    pl.semaphore_wait(stage_ready.at[at], 1)

    for i, up_there, down_there, axis in neighbours:

        @pl.when(up_there)
        def _():
            pl.semaphore_wait(next_ready.at[i], 1)

    @pl.when(has_next)
    def _():
        depth_up().start()

    @pl.when(has_last)
    def _():
        depth_down().start()

    if n_freq > 1:
        start_pair(sh_copies())

    row = lax.broadcasted_iota(jnp.int32, (rows, CHUNK), 0)
    offset = jnp.where(row >= rows - HALO, row - rows, row)
    angle = ((dir_at * dir_local + offset).astype(jnp.float32) + 0.5) * (2.0 * math.pi / DIR)
    trig[0] = jnp.sin(angle)
    trig[1] = jnp.cos(angle)
    half = lax.broadcasted_iota(jnp.int32, (DIR // 2, LANES), 0)
    half_angle = (half.astype(jnp.float32) + 0.5) * (2.0 * math.pi / DIR)
    half_sin, half_cos = jnp.sin(half_angle), jnp.cos(half_angle)
    for copy in loads:
        copy.wait()
    wet = wet_ref[...].astype(jnp.float32)
    trig_row = (jnp.sin(slope_ref[...]), jnp.cos(slope_ref[...]), jnp.sin(heading_ref[...]), jnp.cos(heading_ref[...]))
    turn_row[1:2, :] = trig_row[0]
    turn_row[2:3, :] = trig_row[1]
    shift_row[1:2, :] = trig_row[2]
    shift_row[2:3, :] = trig_row[3]

    @pl.when(jnp.logical_not(has_below))
    def _():
        @pl.loop(0, HALO)
        def _(f):
            ext[f] = jnp.zeros((dir_local, points), jnp.float32)

    @pl.when(jnp.logical_not(has_above))
    def _():
        @pl.loop(freq_local + HALO, freq_local + 2 * HALO)
        def _(f):
            ext[f] = jnp.zeros((dir_local, points), jnp.float32)

    @pl.when(has_next)
    def _():
        depth_up().wait_send()
        depth_down().wait_recv()

    @pl.when(has_last)
    def _():
        depth_down().wait_send()
        depth_up().wait_recv()

    depth = depth_ref[...]
    lane = lax.broadcasted_iota(jnp.int32, (1, points), 1)
    before = jnp.where(pts_at == 0, depth[:, :1], depth_in[0][:, LANES - 1 :])
    after = jnp.where(pts_at == n_pts - 1, depth[:, points - 1 :], depth_in[1][:, :1])
    left = jnp.where(lane == 0, before, pltpu.roll(depth, 1, 1))
    right = jnp.where(lane == points - 1, after, pltpu.roll(depth, points - 1, 1))
    slope = (right - left) * 0.5 * wet
    turn_row[0:1, :] = slope
    shift_row[0:1, :] = wet

    def peak_step(i, carry):
        turn, shift = carry
        part = pl.ds(pl.multiple_of(i * LANES, LANES), LANES)
        sines = jnp.abs(half_sin * turn_row[2:3, part] - half_cos * turn_row[1:2, part])
        cosines = jnp.abs(half_cos * shift_row[2:3, part] + half_sin * shift_row[1:2, part])
        turn_peak = jnp.max(sines, axis=0, keepdims=True) * jnp.abs(turn_row[0:1, part])
        shift_peak = jnp.max(cosines, axis=0, keepdims=True) * shift_row[0:1, part]
        turn = jnp.maximum(turn, jnp.abs(refraction_ref[:, part]) * turn_peak)
        shift = jnp.maximum(shift, jnp.abs(shifting_ref[:, part]) * shift_peak)
        return turn, shift

    zero = jnp.zeros((freq_local, LANES), jnp.float32)
    turn, shift = lax.fori_loop(0, points // LANES, peak_step, (zero, zero))
    turn = jnp.max(jnp.max(turn, axis=0, keepdims=True), axis=1, keepdims=True)
    shift = jnp.max(jnp.max(shift, axis=0, keepdims=True), axis=1, keepdims=True)
    tile = lax.broadcasted_iota(jnp.int32, (SUB, LANES), 0)
    peaks[0] = jnp.where(tile < SUB // 2, turn, shift)

    def peak_copy(source, slot, move):
        return remote(
            peaks.at[source], peaks.at[slot], peak_send.at[slot], peak_recv.at[slot], partner(*move)
        )

    slots, taken = [], 1
    for stage in stages:
        slots.append((taken - 1, [(taken + i, move) for i, move in enumerate(stage)]))
        taken += len(stage) + 1
    for slot, move in slots[0][1] if slots else []:
        peak_copy(0, slot, move).start()

    for block in range(points // BLK):
        part = pl.ds(block * BLK, BLK)
        count_row[0:1, part] = jnp.broadcast_to(
            substeps_ref[0:1, block : block + 1].astype(jnp.float32), (1, BLK)
        )
    count = count_row[0:1, :]
    for k in range(1, KMAX):
        count_row[k : k + 1, :] = jnp.where(count > k, 1.0, 0.0)

    if n_freq > 1:
        wait_pair(sh_copies())
    face_rows = freq_local + 2 * HALO
    first = freq_at * freq_local - HALO

    @pl.loop(0, points // CHUNK)
    def _(c):
        part = span(c)
        window = jnp.concatenate(
            [shext[0, :, part][SUB - HALO :], shifting_ref[:, part], shext[1, :, part][:HALO]], axis=0
        )
        following = jnp.concatenate([window[1:], window[:1]], axis=0)
        mark = first + lax.broadcasted_iota(jnp.int32, (face_rows, CHUNK), 0)
        valid = (mark >= 0) & (mark + 1 <= FREQ - 1)
        face = jnp.where(valid, 0.5 * (window + following), 0.0)
        face_shift[:face_rows, :, part] = face[:, None, :]
        for k in range(1, KMAX):
            face_shift[k * face_rows : (k + 1) * face_rows, :, part] = (face * count_row[k : k + 1, part])[:, None, :]

    top = peaks[0]
    for at, (source, moves) in enumerate(slots):
        for slot, move in moves:
            if at:
                peak_copy(source, slot, move).start()
        for slot, move in moves:
            peak_copy(source, slot, move).wait()
            top = jnp.maximum(top, peaks[slot])
        if at + 1 < len(slots):
            peaks[slots[at + 1][0]] = top
    scale_turn = 0.5 / (top[0:1, 0:1] + EPSILON)
    scale_shift = 0.5 / (top[SUB // 2 : SUB // 2 + 1, 0:1] + EPSILON)
    turn_row[0:1, :] = turn_row[0:1, :] * scale_turn / count
    shift_row[3:4, :] = shift_row[0:1, :] * scale_shift / count

    def active_of(part):
        return [None] + [count_row[k : k + 1, part] for k in range(1, KMAX)]

    def turn_face(part):
        speed = (trig[0] * turn_row[2:3, part] - trig[1] * turn_row[1:2, part]) * turn_row[0:1, part]
        return 0.5 * (speed + pltpu.roll(speed, rows - 1, 0))

    def shift_speed(part):
        width = part.size
        return (
            trig[1, :dir_local, :width] * shift_row[2:3, part] + trig[0, :dir_local, :width] * shift_row[1:2, part]
        ) * shift_row[3:4, part]

    def turn_some(c, start, size):
        part = span(c)
        face = turn_face(part)
        forward = face > 0.0
        active = active_of(part)

        def one(f):
            ext[HALO + f, :, part] = turn_row_of(
                f, part, own, halo, refraction_ref, face, forward, active, rows, dir_local
            )

        @pl.loop(0, size // 2)
        def _(i):
            one(start + 2 * i)
            one(start + 2 * i + 1)

    def shift_chunk(c):
        @pl.loop(0, CHUNK // LANES)
        def _(h):
            part = pl.ds(pl.multiple_of(c * CHUNK + h * LANES, LANES), LANES)

            def store(f, value):
                out_ref[f, :, part] = value

            shift_columns(
                part,
                ext,
                lambda k, q: face_shift[k * face_rows + q, :, part],
                shift_speed(part),
                shift_row[0:1, part],
                store,
                face_rows,
            )

    per_piece = chunks // PIECES

    @pl.loop(0, PIECES)
    def _(i):
        for e in range(len(edges)):
            for way in range(2):
                edge_copy(way, e, i).wait()

        @pl.loop(0, per_piece)
        def _(c):
            for start in edges:
                turn_some(i * per_piece + c, start, HALO)

        if n_freq > 1:
            start_pair(freq_copies(i))

    @pl.loop(0, PIECES)
    def _(i):
        if n_freq > 1:
            wait_pair(freq_copies(i))

        @pl.loop(0, jnp.where(i == PIECES - 1, per_piece - 1, per_piece))
        def _(j):
            c = i * per_piece + j
            for way in range(2):
                dir_copy(way, c).wait()
            turn_some(c, inner, inner_size)
            shift_chunk(c)

    end = span(chunks - 1)
    tail_own[...] = own[:, :, end]
    tail_ext[...] = ext[:, :, end]
    tail_refraction[...] = refraction_ref[:, end]
    tail_face[...] = turn_face(end)
    tail_speed[...] = shift_speed(end)
    tail_steps[...] = face_shift[:, :, end]
    for k in range(1, KMAX):
        tail_rows[k : k + 1, :] = count_row[k : k + 1, end]
    tail_rows[0:1, :] = shift_row[0:1, end]
    for way in range(2):
        dir_copy(way, chunks - 1).wait()
    tail_halo[...] = halo[:, :, end]


def finish(
    n_freq,
    done,
    tail_own,
    tail_halo,
    tail_ext,
    tail_refraction,
    tail_face,
    tail_speed,
    tail_steps,
    tail_rows,
    out_hbm,
    ext,
    last,
    main_sem,
    last_sem,
):
    freq_local, dir_local, points = done.shape
    width = tail_own.shape[2]
    rows = tail_face.shape[0]
    pieces = main_sem.shape[0]
    each = freq_local // pieces
    head = points - width

    def main_copy(i):
        freqs = pl.ds(i * each, each)
        at = pl.ds(0, head)
        return pltpu.make_async_copy(done.at[freqs, :, at], out_hbm.at[freqs, :, at], main_sem.at[i])

    for i in range(pieces):
        main_copy(i).start()

    freq_at = lax.axis_index("freq")
    if n_freq == 1:
        inner, inner_size = 0, freq_local
    elif n_freq == 2:
        inner, inner_size = jnp.where(freq_at < n_freq - 1, 0, HALO), freq_local - HALO
    else:
        inner, inner_size = HALO, freq_local - 2 * HALO

    ext[...] = tail_ext[...]
    everything = pl.ds(0, width)
    face = tail_face[...]
    forward = face > 0.0
    active = [None] + [tail_rows[k : k + 1, :] for k in range(1, KMAX)]

    def one(f):
        ext[HALO + f] = turn_row_of(
            f, everything, tail_own, tail_halo, tail_refraction, face, forward, active, rows, dir_local
        )

    @pl.loop(0, inner_size // 2)
    def _(i):
        one(inner + 2 * i)
        one(inner + 2 * i + 1)

    @pl.loop(0, width // LANES)
    def _(h):
        part = pl.ds(pl.multiple_of(h * LANES, LANES), LANES)

        def store(f, value):
            last[f, :, part] = value

        shift_columns(
            part,
            ext,
            lambda k, q: tail_steps[k * (freq_local + 2 * HALO) + q, :, part],
            tail_speed[:, part],
            tail_rows[0:1, part],
            store,
            freq_local + 2 * HALO,
        )

    final = pltpu.make_async_copy(last, out_hbm.at[:, :, pl.ds(head, width)], last_sem)
    final.start()
    for i in range(pieces):
        main_copy(i).wait()
    final.wait()


def local(mesh, action, bathymetry, refraction, shifting, heading, slope_angle, wet_mask, substeps):
    freq_local, dir_local, points = action.shape
    n_pts, n_dir, n_freq = mesh.shape["pts"], mesh.shape["dir"], mesh.shape["freq"]
    chunks = points // CHUNK
    rows = -(-(dir_local + 2 * HALO) // SUB) * SUB
    face_rows = freq_local + 2 * HALO
    stages = peak_stages(n_pts, n_freq)
    n_slots = 1 + sum(len(stage) + 1 for stage in stages)
    vmem = pl.BlockSpec(memory_space=pltpu.VMEM)
    hbm = pl.BlockSpec(memory_space=pltpu.HBM)
    dma = pltpu.SemaphoreType.DMA
    f32 = jnp.float32
    n_edges = max(1, min(2, n_freq - 1))
    shapes = [
        (freq_local, dir_local, points),
        (freq_local, dir_local, CHUNK),
        (freq_local, 2 * HALO, CHUNK),
        (face_rows, dir_local, CHUNK),
        (freq_local, CHUNK),
        (rows, CHUNK),
        (dir_local, CHUNK),
        (KMAX * face_rows, 1, CHUNK),
        (SUB, CHUNK),
    ]
    parts = pl.pallas_call(
        functools.partial(kernel, n_pts, n_dir, n_freq),
        out_shape=[jax.ShapeDtypeStruct(shape, f32) for shape in shapes],
        in_specs=[hbm] * 8,
        out_specs=[vmem] * len(shapes),
        scratch_shapes=[
            pltpu.VMEM((freq_local, dir_local, points), f32),
            pltpu.VMEM((freq_local, 2 * HALO, points), f32),
            pltpu.VMEM((face_rows, dir_local, points), f32),
            pltpu.VMEM((2, SUB, points), f32),
            pltpu.VMEM((KMAX * face_rows, 1, points), f32),
            pltpu.VMEM((1, points), f32),
            pltpu.VMEM((freq_local, points), f32),
            pltpu.VMEM((freq_local, points), f32),
            pltpu.VMEM((1, points), f32),
            pltpu.VMEM((1, points), f32),
            pltpu.VMEM((1, points), jnp.int32),
            pltpu.VMEM((1, points // BLK), jnp.int32),
            pltpu.VMEM((SUB, points), f32),
            pltpu.VMEM((SUB, points), f32),
            pltpu.VMEM((SUB, points), f32),
            pltpu.VMEM((2, rows, CHUNK), f32),
            pltpu.VMEM((2, 1, LANES), f32),
            pltpu.VMEM((n_slots, SUB, LANES), f32),
            dma((PIECES,)),
            dma((n_edges, PIECES)),
            dma((7,)),
            dma((2, n_edges, PIECES)),
            dma((2, n_edges, PIECES)),
            dma((2, chunks)),
            dma((2, chunks)),
            dma((2, PIECES)),
            dma((2, PIECES)),
            dma((2,)),
            dma((2,)),
            dma((2,)),
            dma((2,)),
            dma((n_slots,)),
            dma((n_slots,)),
            pltpu.SemaphoreType.REGULAR,
            pltpu.SemaphoreType.REGULAR((max(1, len(stages)),)),
            pltpu.SemaphoreType.REGULAR((2,)),
        ],
        compiler_params=pltpu.CompilerParams(
            collective_id=0, has_side_effects=True, vmem_limit_bytes=44 * 1024 * 1024
        ),
    )(
        *[
            pltpu.with_memory_space_constraint(array, pltpu.HBM)
            for array in (
                action,
                bathymetry.reshape(1, points),
                refraction,
                shifting,
                heading.reshape(1, points),
                slope_angle.reshape(1, points),
                wet_mask.reshape(1, points),
                substeps.reshape(1, -1),
            )
        ]
    )
    return pl.pallas_call(
        functools.partial(finish, n_freq),
        out_shape=jax.ShapeDtypeStruct(action.shape, f32),
        in_specs=[vmem] * len(shapes),
        out_specs=hbm,
        scratch_shapes=[
            pltpu.VMEM((face_rows, dir_local, CHUNK), f32),
            pltpu.VMEM((freq_local, dir_local, CHUNK), f32),
            dma((6,)),
            dma(()),
        ],
        compiler_params=pltpu.CompilerParams(vmem_limit_bytes=8 * 1024 * 1024),
    )(*parts)


def solution(mesh):
    placed = (
        P("freq", "dir", "pts"),
        P("pts"),
        P("freq", "pts"),
        P("freq", "pts"),
        P("pts"),
        P("pts"),
        P("pts"),
        P("pts"),
    )
    return jax.shard_map(
        functools.partial(local, mesh),
        mesh=mesh,
        in_specs=placed,
        out_specs=P("freq", "dir", "pts"),
        check_vma=False,
    )
```

```python
import functools
import math

import jax
import jax.numpy as jnp
from jax import lax
from jax.experimental import pallas as pl
from jax.experimental.pallas import tpu as pltpu
from jax.sharding import PartitionSpec as P

FREQ = 48
DIR = 64
KMAX = 4
BLK = 512
CHUNK = 256
LANES = 128
HALO = KMAX
SUB = 8
PIECES = 2
LEAD = 1

EPSILON = 1e-06
MESH = pl.DeviceIdType.MESH


def turn_row_of(f, part, own, halo, refraction, face, forward, active, rows, dir_local):
    spare = rows - dir_local - 2 * HALO
    if spare:
        cells = jnp.concatenate(
            [
                own[f, :, part],
                halo[f, :HALO, part],
                jnp.zeros((spare, face.shape[1]), jnp.float32),
                halo[f, HALO:, part],
            ],
            axis=0,
        )
    else:
        cells = jnp.concatenate([own[f, :, part], halo[f, :, part]], axis=0)
    rate = refraction[pl.ds(f, 1), part]
    for k in range(KMAX):
        flux = face * jnp.where(forward, cells, pltpu.roll(cells, rows - 1, 0))
        step = rate if k == 0 else rate * active[k]
        cells = cells - step * (flux - pltpu.roll(flux, 1, 0))
    return cells[:dir_local]


def shift_columns(part, ext, face_at, speed, wet, store, size):
    forward = speed > 0.0
    here, flux, out = [None] * KMAX, [None] * KMAX, [None] * KMAX

    def advance(t, k, there, skip_out=False):
        q = t - 2 * k
        beyond = face_at(k, q) * (speed * jnp.where(forward, here[k], there))
        cells = None if skip_out else here[k] - (beyond - flux[k])
        here[k], flux[k] = there, beyond
        return cells

    def ramp(t):
        before = list(out)
        for k in range(KMAX):
            q = t - 2 * k
            if q < k - 1 or q > size - 2 - k:
                continue
            there = ext[q + 1, :, part] if k == 0 else before[k - 1]
            if q == k - 1:
                here[k] = there
            elif q == k:
                advance(t, k, there, skip_out=True)
            else:
                out[k] = advance(t, k, there)
                if k == KMAX - 1:
                    store(q - HALO, out[k] * wet)

    here[0] = ext[0, :, part]
    first = 3 * (KMAX - 1) + 1
    last = size - 1
    for t in range(first):
        ramp(t)

    def step(t, carry):
        now_here, now_flux, now_out = carry
        here[:], flux[:] = list(now_here), list(now_flux)
        fresh = []
        for k in range(KMAX):
            there = ext[t + 1, :, part] if k == 0 else now_out[k - 1]
            fresh.append(advance(t, k, there))
        store(t - 2 * (KMAX - 1) - HALO, fresh[KMAX - 1] * wet)
        return tuple(here), tuple(flux), tuple(fresh[: KMAX - 1])

    trips = last - first
    unroll = 3 if trips % 3 == 0 else 1
    state = lax.fori_loop(first, last, step, (tuple(here), tuple(flux), tuple(out[: KMAX - 1])), unroll=unroll)
    here[:], flux[:], out[: KMAX - 1] = list(state[0]), list(state[1]), list(state[2])
    for t in range(last, size - KMAX + 2 * (KMAX - 1)):
        ramp(t)


def peak_stages(n_pts, n_freq):
    stages = []
    for axis, count in (("pts", n_pts), ("freq", n_freq)):
        if count & (count - 1) == 0:
            amount = 1
            while amount < count:
                stages.append([(axis, "swap", amount)])
                amount *= 2
        else:
            stages.append([(axis, "turn", amount) for amount in range(1, count)])
    return stages


def kernel(
    n_pts,
    n_dir,
    n_freq,
    action_ref,
    depth_hbm,
    refraction_hbm,
    shifting_hbm,
    heading_hbm,
    slope_hbm,
    wet_hbm,
    substeps_hbm,
    out_ref,
    tail_own,
    tail_halo,
    tail_ext,
    tail_refraction,
    tail_face,
    tail_speed,
    tail_steps,
    tail_rows,
    own,
    halo,
    ext,
    shext,
    face_shift,
    depth_ref,
    refraction_ref,
    shifting_ref,
    heading_ref,
    slope_ref,
    wet_ref,
    substeps_ref,
    turn_row,
    shift_row,
    count_row,
    trig,
    depth_in,
    peaks,
    own_sem,
    own_edge_sem,
    load_sem,
    edge_send,
    edge_recv,
    dir_send,
    dir_recv,
    freq_send,
    freq_recv,
    sh_send,
    sh_recv,
    depth_send,
    depth_recv,
    peak_send,
    peak_recv,
    dir_ready,
    stage_ready,
    next_ready,
):
    freq_local, dir_local, points = own.shape
    chunks = points // CHUNK
    piece = points // PIECES
    rows = -(-(dir_local + 2 * HALO) // SUB) * SUB
    pts_at = lax.axis_index("pts")
    dir_at = lax.axis_index("dir")
    freq_at = lax.axis_index("freq")
    dir_up, dir_down = lax.rem(dir_at + 1, n_dir), lax.rem(dir_at + n_dir - 1, n_dir)
    has_above = freq_at < n_freq - 1
    has_below = freq_at > 0
    has_next = pts_at < n_pts - 1
    has_last = pts_at > 0
    stages = peak_stages(n_pts, n_freq)
    places = {"pts": (pts_at, n_pts), "freq": (freq_at, n_freq)}

    def partner(axis, kind, amount):
        at, count = places[axis]
        if kind == "swap":
            return {axis: at + amount * (1 - 2 * lax.rem(lax.div(at, amount), 2))}
        return {axis: lax.rem(at + amount, count)}

    def bit(axis, amount):
        return lax.rem(lax.div(places[axis][0], amount), 2)

    neighbours = [(0, has_next, has_last, "pts")]
    if n_freq > 2:
        neighbours.append((1, has_above, has_below, "freq"))
    barrier = pltpu.get_barrier_semaphore()

    def greet(where):
        pl.semaphore_signal(barrier, inc=1, device_id=where, device_id_type=MESH)

    last_dir = n_dir - 1

    @pl.when(dir_at < last_dir)
    def _():
        greet({"dir": dir_up})

    @pl.when(dir_at == 1)
    def _():
        greet({"dir": dir_down})

    @pl.when(dir_at == 0)
    def _():
        greet({"dir": dir_down})

    parents = 1 + lax.div(dir_at, last_dir)
    for stage in stages:
        for axis, kind, amount in stage:
            if kind == "swap":
                pl.when(bit(axis, amount) == 0)(functools.partial(greet, partner(axis, kind, amount)))
                parents += bit(axis, amount)
            else:
                greet(partner(axis, kind, amount))
                parents += 1
    for _, up_there, _, axis in neighbours:
        pl.when(up_there)(functools.partial(greet, {axis: places[axis][0] + 1}))
        parents += jnp.minimum(places[axis][0], 1)

    if n_freq == 1:
        edges = []
        inner, inner_size = 0, freq_local
    elif n_freq == 2:
        edges = [jnp.where(has_above, freq_local - HALO, 0)]
        inner, inner_size = jnp.where(has_above, 0, HALO), freq_local - HALO
    else:
        edges = [0, freq_local - HALO]
        inner, inner_size = HALO, freq_local - 2 * HALO

    def span(c):
        return pl.ds(pl.multiple_of(c * CHUNK, CHUNK), CHUNK)

    def piece_span(i):
        return pl.ds(pl.multiple_of(i * piece, piece), piece)

    def own_part(freqs, i, sem):
        at = piece_span(i)
        return pltpu.make_async_copy(action_ref.at[freqs, :, at], own.at[freqs, :, at], sem)

    def own_edge(e, i):
        return own_part(pl.ds(edges[e], HALO), i, own_edge_sem.at[e, i])

    def own_inner(i):
        return own_part(pl.ds(inner, inner_size), i, own_sem.at[i])

    for i in range(PIECES):
        for e in range(len(edges)):
            own_edge(e, i).start()
    for i in range(PIECES):
        own_inner(i).start()

    loads = [
        pltpu.make_async_copy(source, target, load_sem.at[i])
        for i, (source, target) in enumerate(
            (
                (slope_hbm, slope_ref),
                (heading_hbm, heading_ref),
                (depth_hbm, depth_ref),
                (wet_hbm, wet_ref),
                (refraction_hbm, refraction_ref),
                (shifting_hbm, shifting_ref),
                (substeps_hbm, substeps_ref),
            )
        )
    ]
    for copy in loads:
        copy.start()

    def remote(src, dst, send, recv, where):
        return pltpu.make_async_remote_copy(
            src_ref=src, dst_ref=dst, send_sem=send, recv_sem=recv, device_id=where, device_id_type=MESH
        )

    def depth_up():
        return remote(
            depth_hbm.at[:, pl.ds(points - LANES, LANES)],
            depth_in.at[0],
            depth_send.at[0],
            depth_recv.at[0],
            {"pts": pts_at + 1},
        )

    def depth_down():
        return remote(
            depth_hbm.at[:, pl.ds(0, LANES)],
            depth_in.at[1],
            depth_send.at[1],
            depth_recv.at[1],
            {"pts": pts_at - 1},
        )

    def halo_copy(way, freqs, at, send, recv):
        top = pl.ds(dir_local - HALO, HALO)
        source, target, where = (top, pl.ds(HALO, HALO), dir_up) if way == 0 else (
            pl.ds(0, HALO),
            pl.ds(0, HALO),
            dir_down,
        )
        return remote(own.at[freqs, source, at], halo.at[freqs, target, at], send, recv, {"dir": where})

    def edge_copy(way, e, i):
        return halo_copy(
            way, pl.ds(edges[e], HALO), piece_span(i), edge_send.at[way, e, i], edge_recv.at[way, e, i]
        )

    def dir_copy(way, c):
        return halo_copy(way, pl.ds(inner, inner_size), span(c), dir_send.at[way, c], dir_recv.at[way, c])

    above, below = lax.rem(freq_at + 1, n_freq), lax.rem(freq_at + n_freq - 1, n_freq)

    def rise(src, dst, send, recv):
        return remote(src, dst, send, recv, {"freq": above})

    def fall(src, dst, send, recv):
        return remote(src, dst, send, recv, {"freq": below})

    def freq_copies(i):
        at = piece_span(i)
        return (
            rise(
                ext.at[pl.ds(freq_local, HALO), :, at],
                ext.at[pl.ds(0, HALO), :, at],
                freq_send.at[0, i],
                freq_recv.at[0, i],
            ),
            fall(
                ext.at[pl.ds(HALO, HALO), :, at],
                ext.at[pl.ds(freq_local + HALO, HALO), :, at],
                freq_send.at[1, i],
                freq_recv.at[1, i],
            ),
        )

    def sh_copies():
        return (
            rise(
                shifting_hbm.at[pl.ds(freq_local - SUB, SUB)],
                shext.at[0],
                sh_send.at[0],
                sh_recv.at[0],
            ),
            fall(shifting_hbm.at[pl.ds(0, SUB)], shext.at[1], sh_send.at[1], sh_recv.at[1]),
        )

    def start_pair(pair):
        @pl.when(has_above)
        def _():
            pair[0].start()

        @pl.when(has_below)
        def _():
            pair[1].start()

    def wait_pair(pair):
        @pl.when(has_above)
        def _():
            pair[0].wait_send()
            pair[1].wait_recv()

        @pl.when(has_below)
        def _():
            pair[1].wait_send()
            pair[0].wait_recv()

    def report(sem, where):
        pl.semaphore_signal(sem, inc=1, device_id=where, device_id_type=MESH)

    pl.semaphore_wait(barrier, parents)

    @pl.when(dir_at > 1)
    def _():
        report(dir_ready, {"dir": dir_down})

    @pl.when(dir_at == last_dir)
    def _():
        report(dir_ready, {"dir": dir_up})

    for at, stage in enumerate(stages):
        for axis, kind, amount in stage:
            if kind == "swap":
                below_there = bit(axis, amount) == 1
                pl.when(below_there)(functools.partial(report, stage_ready.at[at], partner(axis, kind, amount)))
    for i, up_there, down_there, axis in neighbours:
        pl.when(down_there)(functools.partial(report, next_ready.at[i], {axis: places[axis][0] - 1}))
    def start_edges(way, low=0, high=PIECES):
        for i in range(low, high):
            for e in range(len(edges)):
                edge_copy(way, e, i).start()

    def start_inner(first, ahead):
        for c in range(ahead):
            dir_copy(first, c).start()

        @pl.loop(0, chunks - ahead)
        def _(c):
            dir_copy(first, c + ahead).start()
            dir_copy(1 - first, c).start()

        for c in range(chunks - ahead, chunks):
            dir_copy(1 - first, c).start()

    for i in range(PIECES):
        for e in range(len(edges)):
            own_edge(e, i).wait()

    is_end = (dir_at == 0) | (dir_at == last_dir)

    @pl.when(dir_at == 0)
    def _():
        start_edges(0, 0, 1)

    @pl.when(dir_at == last_dir)
    def _():
        start_edges(0, 0, 1)

    @pl.when(jnp.logical_not(is_end))
    def _():
        start_edges(1)


    @pl.when(dir_at < last_dir)
    def _():
        pl.semaphore_wait(dir_ready, 1)

    for i in range(PIECES):
        own_inner(i).wait()

    @pl.when(dir_at == 0)
    def _():
        for i in range(PIECES):
            start_edges(1, i, i + 1)
            if i + 1 < PIECES:
                start_edges(0, i + 1, i + 2)
        start_inner(1, 3)

    @pl.when(dir_at == last_dir)
    def _():
        for i in range(PIECES):
            start_edges(1, i, i + 1)
            if i + 1 < PIECES:
                start_edges(0, i + 1, i + 2)
        start_inner(0, LEAD)

    @pl.when(jnp.logical_not(is_end))
    def _():
        start_edges(0)
        start_inner(0, 0)

    for at, stage in enumerate(stages):
        for axis, kind, amount in stage:
            if kind == "swap":

                @pl.when(bit(axis, amount) == 0)
                def _():
                    pl.semaphore_wait(stage_ready.at[at], 1)

    for i, up_there, down_there, axis in neighbours:

        @pl.when(up_there)
        def _():
            pl.semaphore_wait(next_ready.at[i], 1)

    @pl.when(has_next)
    def _():
        depth_up().start()

    @pl.when(has_last)
    def _():
        depth_down().start()

    if n_freq > 1:
        start_pair(sh_copies())

    row = lax.broadcasted_iota(jnp.int32, (rows, CHUNK), 0)
    offset = jnp.where(row >= rows - HALO, row - rows, row)
    angle = ((dir_at * dir_local + offset).astype(jnp.float32) + 0.5) * (2.0 * math.pi / DIR)
    trig[0] = jnp.sin(angle)
    trig[1] = jnp.cos(angle)
    half = lax.broadcasted_iota(jnp.int32, (DIR // 2, LANES), 0)
    half_angle = (half.astype(jnp.float32) + 0.5) * (2.0 * math.pi / DIR)
    half_sin, half_cos = jnp.sin(half_angle), jnp.cos(half_angle)
    for copy in loads:
        copy.wait()
    wet = wet_ref[...].astype(jnp.float32)
    trig_row = (jnp.sin(slope_ref[...]), jnp.cos(slope_ref[...]), jnp.sin(heading_ref[...]), jnp.cos(heading_ref[...]))
    turn_row[1:2, :] = trig_row[0]
    turn_row[2:3, :] = trig_row[1]
    shift_row[1:2, :] = trig_row[2]
    shift_row[2:3, :] = trig_row[3]

    @pl.when(jnp.logical_not(has_below))
    def _():
        @pl.loop(0, HALO)
        def _(f):
            ext[f] = jnp.zeros((dir_local, points), jnp.float32)

    @pl.when(jnp.logical_not(has_above))
    def _():
        @pl.loop(freq_local + HALO, freq_local + 2 * HALO)
        def _(f):
            ext[f] = jnp.zeros((dir_local, points), jnp.float32)

    @pl.when(has_next)
    def _():
        depth_up().wait_send()
        depth_down().wait_recv()

    @pl.when(has_last)
    def _():
        depth_down().wait_send()
        depth_up().wait_recv()

    depth = depth_ref[...]
    lane = lax.broadcasted_iota(jnp.int32, (1, points), 1)
    before = jnp.where(pts_at == 0, depth[:, :1], depth_in[0][:, LANES - 1 :])
    after = jnp.where(pts_at == n_pts - 1, depth[:, points - 1 :], depth_in[1][:, :1])
    left = jnp.where(lane == 0, before, pltpu.roll(depth, 1, 1))
    right = jnp.where(lane == points - 1, after, pltpu.roll(depth, points - 1, 1))
    slope = (right - left) * 0.5 * wet
    turn_row[0:1, :] = slope
    shift_row[0:1, :] = wet

    def peak_step(i, carry):
        turn, shift = carry
        part = pl.ds(pl.multiple_of(i * LANES, LANES), LANES)
        sines = jnp.abs(half_sin * turn_row[2:3, part] - half_cos * turn_row[1:2, part])
        cosines = jnp.abs(half_cos * shift_row[2:3, part] + half_sin * shift_row[1:2, part])
        turn_peak = jnp.max(sines, axis=0, keepdims=True) * jnp.abs(turn_row[0:1, part])
        shift_peak = jnp.max(cosines, axis=0, keepdims=True) * shift_row[0:1, part]
        turn = jnp.maximum(turn, jnp.abs(refraction_ref[:, part]) * turn_peak)
        shift = jnp.maximum(shift, jnp.abs(shifting_ref[:, part]) * shift_peak)
        return turn, shift

    zero = jnp.zeros((freq_local, LANES), jnp.float32)
    turn, shift = lax.fori_loop(0, points // LANES, peak_step, (zero, zero))
    turn = jnp.max(jnp.max(turn, axis=0, keepdims=True), axis=1, keepdims=True)
    shift = jnp.max(jnp.max(shift, axis=0, keepdims=True), axis=1, keepdims=True)
    tile = lax.broadcasted_iota(jnp.int32, (SUB, LANES), 0)
    peaks[0] = jnp.where(tile < SUB // 2, turn, shift)

    def peak_copy(source, slot, move):
        return remote(
            peaks.at[source], peaks.at[slot], peak_send.at[slot], peak_recv.at[slot], partner(*move)
        )

    slots, taken = [], 1
    for stage in stages:
        slots.append((taken - 1, [(taken + i, move) for i, move in enumerate(stage)]))
        taken += len(stage) + 1
    for slot, move in slots[0][1] if slots else []:
        peak_copy(0, slot, move).start()

    for block in range(points // BLK):
        part = pl.ds(block * BLK, BLK)
        count_row[0:1, part] = jnp.broadcast_to(
            substeps_ref[0:1, block : block + 1].astype(jnp.float32), (1, BLK)
        )
    count = count_row[0:1, :]
    for k in range(1, KMAX):
        count_row[k : k + 1, :] = jnp.where(count > k, 1.0, 0.0)

    if n_freq > 1:
        wait_pair(sh_copies())
    face_rows = freq_local + 2 * HALO
    first = freq_at * freq_local - HALO

    @pl.loop(0, points // CHUNK)
    def _(c):
        part = span(c)
        window = jnp.concatenate(
            [shext[0, :, part][SUB - HALO :], shifting_ref[:, part], shext[1, :, part][:HALO]], axis=0
        )
        following = jnp.concatenate([window[1:], window[:1]], axis=0)
        mark = first + lax.broadcasted_iota(jnp.int32, (face_rows, CHUNK), 0)
        valid = (mark >= 0) & (mark + 1 <= FREQ - 1)
        face = jnp.where(valid, 0.5 * (window + following), 0.0)
        face_shift[:face_rows, :, part] = face[:, None, :]
        for k in range(1, KMAX):
            face_shift[k * face_rows : (k + 1) * face_rows, :, part] = (face * count_row[k : k + 1, part])[:, None, :]

    top = peaks[0]
    for at, (source, moves) in enumerate(slots):
        for slot, move in moves:
            if at:
                peak_copy(source, slot, move).start()
        for slot, move in moves:
            peak_copy(source, slot, move).wait()
            top = jnp.maximum(top, peaks[slot])
        if at + 1 < len(slots):
            peaks[slots[at + 1][0]] = top
    scale_turn = 0.5 / (top[0:1, 0:1] + EPSILON)
    scale_shift = 0.5 / (top[SUB // 2 : SUB // 2 + 1, 0:1] + EPSILON)
    turn_row[0:1, :] = turn_row[0:1, :] * scale_turn / count
    shift_row[3:4, :] = shift_row[0:1, :] * scale_shift / count

    def active_of(part):
        return [None] + [count_row[k : k + 1, part] for k in range(1, KMAX)]

    def turn_face(part):
        speed = (trig[0] * turn_row[2:3, part] - trig[1] * turn_row[1:2, part]) * turn_row[0:1, part]
        return 0.5 * (speed + pltpu.roll(speed, rows - 1, 0))

    def shift_speed(part):
        width = part.size
        return (
            trig[1, :dir_local, :width] * shift_row[2:3, part] + trig[0, :dir_local, :width] * shift_row[1:2, part]
        ) * shift_row[3:4, part]

    def turn_some(c, start, size):
        part = span(c)
        face = turn_face(part)
        forward = face > 0.0
        active = active_of(part)

        def one(f):
            ext[HALO + f, :, part] = turn_row_of(
                f, part, own, halo, refraction_ref, face, forward, active, rows, dir_local
            )

        @pl.loop(0, size // 2)
        def _(i):
            one(start + 2 * i)
            one(start + 2 * i + 1)

    def shift_chunk(c):
        @pl.loop(0, CHUNK // LANES)
        def _(h):
            part = pl.ds(pl.multiple_of(c * CHUNK + h * LANES, LANES), LANES)

            def store(f, value):
                out_ref[f, :, part] = value

            shift_columns(
                part,
                ext,
                lambda k, q: face_shift[k * face_rows + q, :, part],
                shift_speed(part),
                shift_row[0:1, part],
                store,
                face_rows,
            )

    per_piece = chunks // PIECES

    @pl.loop(0, PIECES)
    def _(i):
        for e in range(len(edges)):
            for way in range(2):
                edge_copy(way, e, i).wait()

        @pl.loop(0, per_piece)
        def _(c):
            for start in edges:
                turn_some(i * per_piece + c, start, HALO)

        if n_freq > 1:
            start_pair(freq_copies(i))

    @pl.loop(0, PIECES)
    def _(i):
        if n_freq > 1:
            wait_pair(freq_copies(i))

        @pl.loop(0, jnp.where(i == PIECES - 1, per_piece - 1, per_piece))
        def _(j):
            c = i * per_piece + j
            for way in range(2):
                dir_copy(way, c).wait()
            turn_some(c, inner, inner_size)
            shift_chunk(c)

    end = span(chunks - 1)
    tail_own[...] = own[:, :, end]
    tail_ext[...] = ext[:, :, end]
    tail_refraction[...] = refraction_ref[:, end]
    tail_face[...] = turn_face(end)
    tail_speed[...] = shift_speed(end)
    tail_steps[...] = face_shift[:, :, end]
    for k in range(1, KMAX):
        tail_rows[k : k + 1, :] = count_row[k : k + 1, end]
    tail_rows[0:1, :] = shift_row[0:1, end]
    for way in range(2):
        dir_copy(way, chunks - 1).wait()
    tail_halo[...] = halo[:, :, end]


def finish(
    n_freq,
    done,
    tail_own,
    tail_halo,
    tail_ext,
    tail_refraction,
    tail_face,
    tail_speed,
    tail_steps,
    tail_rows,
    out_hbm,
    ext,
    last,
    main_sem,
    last_sem,
):
    freq_local, dir_local, points = done.shape
    width = tail_own.shape[2]
    rows = tail_face.shape[0]
    pieces = main_sem.shape[0]
    each = freq_local // pieces
    head = points - width

    def main_copy(i):
        freqs = pl.ds(i * each, each)
        at = pl.ds(0, head)
        return pltpu.make_async_copy(done.at[freqs, :, at], out_hbm.at[freqs, :, at], main_sem.at[i])

    for i in range(pieces):
        main_copy(i).start()

    freq_at = lax.axis_index("freq")
    if n_freq == 1:
        inner, inner_size = 0, freq_local
    elif n_freq == 2:
        inner, inner_size = jnp.where(freq_at < n_freq - 1, 0, HALO), freq_local - HALO
    else:
        inner, inner_size = HALO, freq_local - 2 * HALO

    ext[...] = tail_ext[...]
    everything = pl.ds(0, width)
    face = tail_face[...]
    forward = face > 0.0
    active = [None] + [tail_rows[k : k + 1, :] for k in range(1, KMAX)]

    def one(f):
        ext[HALO + f] = turn_row_of(
            f, everything, tail_own, tail_halo, tail_refraction, face, forward, active, rows, dir_local
        )

    @pl.loop(0, inner_size // 2)
    def _(i):
        one(inner + 2 * i)
        one(inner + 2 * i + 1)

    @pl.loop(0, width // LANES)
    def _(h):
        part = pl.ds(pl.multiple_of(h * LANES, LANES), LANES)

        def store(f, value):
            last[f, :, part] = value

        shift_columns(
            part,
            ext,
            lambda k, q: tail_steps[k * (freq_local + 2 * HALO) + q, :, part],
            tail_speed[:, part],
            tail_rows[0:1, part],
            store,
            freq_local + 2 * HALO,
        )

    final = pltpu.make_async_copy(last, out_hbm.at[:, :, pl.ds(head, width)], last_sem)
    final.start()
    for i in range(pieces):
        main_copy(i).wait()
    final.wait()


def local(mesh, action, bathymetry, refraction, shifting, heading, slope_angle, wet_mask, substeps):
    freq_local, dir_local, points = action.shape
    n_pts, n_dir, n_freq = mesh.shape["pts"], mesh.shape["dir"], mesh.shape["freq"]
    chunks = points // CHUNK
    rows = -(-(dir_local + 2 * HALO) // SUB) * SUB
    face_rows = freq_local + 2 * HALO
    stages = peak_stages(n_pts, n_freq)
    n_slots = 1 + sum(len(stage) + 1 for stage in stages)
    vmem = pl.BlockSpec(memory_space=pltpu.VMEM)
    hbm = pl.BlockSpec(memory_space=pltpu.HBM)
    dma = pltpu.SemaphoreType.DMA
    f32 = jnp.float32
    n_edges = max(1, min(2, n_freq - 1))
    shapes = [
        (freq_local, dir_local, points),
        (freq_local, dir_local, CHUNK),
        (freq_local, 2 * HALO, CHUNK),
        (face_rows, dir_local, CHUNK),
        (freq_local, CHUNK),
        (rows, CHUNK),
        (dir_local, CHUNK),
        (KMAX * face_rows, 1, CHUNK),
        (SUB, CHUNK),
    ]
    parts = pl.pallas_call(
        functools.partial(kernel, n_pts, n_dir, n_freq),
        out_shape=[jax.ShapeDtypeStruct(shape, f32) for shape in shapes],
        in_specs=[hbm] * 8,
        out_specs=[vmem] * len(shapes),
        scratch_shapes=[
            pltpu.VMEM((freq_local, dir_local, points), f32),
            pltpu.VMEM((freq_local, 2 * HALO, points), f32),
            pltpu.VMEM((face_rows, dir_local, points), f32),
            pltpu.VMEM((2, SUB, points), f32),
            pltpu.VMEM((KMAX * face_rows, 1, points), f32),
            pltpu.VMEM((1, points), f32),
            pltpu.VMEM((freq_local, points), f32),
            pltpu.VMEM((freq_local, points), f32),
            pltpu.VMEM((1, points), f32),
            pltpu.VMEM((1, points), f32),
            pltpu.VMEM((1, points), jnp.int32),
            pltpu.VMEM((1, points // BLK), jnp.int32),
            pltpu.VMEM((SUB, points), f32),
            pltpu.VMEM((SUB, points), f32),
            pltpu.VMEM((SUB, points), f32),
            pltpu.VMEM((2, rows, CHUNK), f32),
            pltpu.VMEM((2, 1, LANES), f32),
            pltpu.VMEM((n_slots, SUB, LANES), f32),
            dma((PIECES,)),
            dma((n_edges, PIECES)),
            dma((7,)),
            dma((2, n_edges, PIECES)),
            dma((2, n_edges, PIECES)),
            dma((2, chunks)),
            dma((2, chunks)),
            dma((2, PIECES)),
            dma((2, PIECES)),
            dma((2,)),
            dma((2,)),
            dma((2,)),
            dma((2,)),
            dma((n_slots,)),
            dma((n_slots,)),
            pltpu.SemaphoreType.REGULAR,
            pltpu.SemaphoreType.REGULAR((max(1, len(stages)),)),
            pltpu.SemaphoreType.REGULAR((2,)),
        ],
        compiler_params=pltpu.CompilerParams(
            collective_id=0, has_side_effects=True, vmem_limit_bytes=44 * 1024 * 1024
        ),
    )(
        *[
            pltpu.with_memory_space_constraint(array, pltpu.HBM)
            for array in (
                action,
                bathymetry.reshape(1, points),
                refraction,
                shifting,
                heading.reshape(1, points),
                slope_angle.reshape(1, points),
                wet_mask.reshape(1, points),
                substeps.reshape(1, -1),
            )
        ]
    )
    return pl.pallas_call(
        functools.partial(finish, n_freq),
        out_shape=jax.ShapeDtypeStruct(action.shape, f32),
        in_specs=[vmem] * len(shapes),
        out_specs=hbm,
        scratch_shapes=[
            pltpu.VMEM((face_rows, dir_local, CHUNK), f32),
            pltpu.VMEM((freq_local, dir_local, CHUNK), f32),
            dma((6,)),
            dma(()),
        ],
        compiler_params=pltpu.CompilerParams(vmem_limit_bytes=8 * 1024 * 1024),
    )(*parts)


def solution(mesh):
    placed = (
        P("freq", "dir", "pts"),
        P("pts"),
        P("freq", "pts"),
        P("freq", "pts"),
        P("pts"),
        P("pts"),
        P("pts"),
        P("pts"),
    )
    return jax.shard_map(
        functools.partial(local, mesh),
        mesh=mesh,
        in_specs=placed,
        out_specs=P("freq", "dir", "pts"),
        check_vma=False,
    )
```

```python
import functools
import math

import jax
import jax.numpy as jnp
from jax import lax
from jax.experimental import pallas as pl
from jax.experimental.pallas import tpu as pltpu
from jax.sharding import PartitionSpec as P

FREQ = 48
DIR = 64
KMAX = 4
BLK = 512
CHUNK = 256
LANES = 128
HALO = KMAX
SUB = 8
PIECES = 2
LEAD = 1

EPSILON = 1e-06
MESH = pl.DeviceIdType.MESH


def turn_row_of(f, part, own, halo, refraction, face, forward, active, rows, dir_local):
    spare = rows - dir_local - 2 * HALO
    if spare:
        cells = jnp.concatenate(
            [
                own[f, :, part],
                halo[f, :HALO, part],
                jnp.zeros((spare, face.shape[1]), jnp.float32),
                halo[f, HALO:, part],
            ],
            axis=0,
        )
    else:
        cells = jnp.concatenate([own[f, :, part], halo[f, :, part]], axis=0)
    rate = refraction[pl.ds(f, 1), part]
    for k in range(KMAX):
        flux = face * jnp.where(forward, cells, pltpu.roll(cells, rows - 1, 0))
        step = rate if k == 0 else rate * active[k]
        cells = cells - step * (flux - pltpu.roll(flux, 1, 0))
    return cells[:dir_local]


def shift_columns(part, ext, face_at, speed, wet, store, size):
    forward = speed > 0.0
    here, flux, out = [None] * KMAX, [None] * KMAX, [None] * KMAX

    def advance(t, k, there, skip_out=False):
        q = t - 2 * k
        beyond = face_at(k, q) * (speed * jnp.where(forward, here[k], there))
        cells = None if skip_out else here[k] - (beyond - flux[k])
        here[k], flux[k] = there, beyond
        return cells

    def ramp(t):
        before = list(out)
        for k in range(KMAX):
            q = t - 2 * k
            if q < k - 1 or q > size - 2 - k:
                continue
            there = ext[q + 1, :, part] if k == 0 else before[k - 1]
            if q == k - 1:
                here[k] = there
            elif q == k:
                advance(t, k, there, skip_out=True)
            else:
                out[k] = advance(t, k, there)
                if k == KMAX - 1:
                    store(q - HALO, out[k] * wet)

    here[0] = ext[0, :, part]
    first = 3 * (KMAX - 1) + 1
    last = size - 1
    for t in range(first):
        ramp(t)

    def step(t, carry):
        now_here, now_flux, now_out = carry
        here[:], flux[:] = list(now_here), list(now_flux)
        fresh = []
        for k in range(KMAX):
            there = ext[t + 1, :, part] if k == 0 else now_out[k - 1]
            fresh.append(advance(t, k, there))
        store(t - 2 * (KMAX - 1) - HALO, fresh[KMAX - 1] * wet)
        return tuple(here), tuple(flux), tuple(fresh[: KMAX - 1])

    trips = last - first
    unroll = 3 if trips % 3 == 0 else 1
    state = lax.fori_loop(first, last, step, (tuple(here), tuple(flux), tuple(out[: KMAX - 1])), unroll=unroll)
    here[:], flux[:], out[: KMAX - 1] = list(state[0]), list(state[1]), list(state[2])
    for t in range(last, size - KMAX + 2 * (KMAX - 1)):
        ramp(t)


def peak_stages(n_pts, n_freq):
    stages = []
    for axis, count in (("pts", n_pts), ("freq", n_freq)):
        if count & (count - 1) == 0:
            amount = 1
            while amount < count:
                stages.append([(axis, "swap", amount)])
                amount *= 2
        else:
            stages.append([(axis, "turn", amount) for amount in range(1, count)])
    return stages


def kernel(
    n_pts,
    n_dir,
    n_freq,
    action_ref,
    depth_hbm,
    refraction_hbm,
    shifting_hbm,
    heading_hbm,
    slope_hbm,
    wet_hbm,
    substeps_hbm,
    out_ref,
    tail_own,
    tail_halo,
    tail_ext,
    tail_refraction,
    tail_face,
    tail_speed,
    tail_steps,
    tail_rows,
    own,
    halo,
    ext,
    shext,
    face_shift,
    depth_ref,
    refraction_ref,
    shifting_ref,
    heading_ref,
    slope_ref,
    wet_ref,
    substeps_ref,
    turn_row,
    shift_row,
    count_row,
    trig,
    depth_in,
    peaks,
    own_sem,
    own_edge_sem,
    load_sem,
    edge_send,
    edge_recv,
    dir_send,
    dir_recv,
    freq_send,
    freq_recv,
    sh_send,
    sh_recv,
    depth_send,
    depth_recv,
    peak_send,
    peak_recv,
    dir_ready,
    stage_ready,
    next_ready,
):
    freq_local, dir_local, points = own.shape
    chunks = points // CHUNK
    piece = points // PIECES
    rows = -(-(dir_local + 2 * HALO) // SUB) * SUB
    pts_at = lax.axis_index("pts")
    dir_at = lax.axis_index("dir")
    freq_at = lax.axis_index("freq")
    dir_up, dir_down = lax.rem(dir_at + 1, n_dir), lax.rem(dir_at + n_dir - 1, n_dir)
    has_above = freq_at < n_freq - 1
    has_below = freq_at > 0
    has_next = pts_at < n_pts - 1
    has_last = pts_at > 0
    stages = peak_stages(n_pts, n_freq)
    places = {"pts": (pts_at, n_pts), "freq": (freq_at, n_freq)}

    def partner(axis, kind, amount):
        at, count = places[axis]
        if kind == "swap":
            return {axis: at + amount * (1 - 2 * lax.rem(lax.div(at, amount), 2))}
        return {axis: lax.rem(at + amount, count)}

    if n_freq == 1:
        edges = []
        inner, inner_size = 0, freq_local
    elif n_freq == 2:
        edges = [jnp.where(has_above, freq_local - HALO, 0)]
        inner, inner_size = jnp.where(has_above, 0, HALO), freq_local - HALO
    else:
        edges = [0, freq_local - HALO]
        inner, inner_size = HALO, freq_local - 2 * HALO

    def span(c):
        return pl.ds(pl.multiple_of(c * CHUNK, CHUNK), CHUNK)

    def piece_span(i):
        return pl.ds(pl.multiple_of(i * piece, piece), piece)

    def own_part(freqs, i, sem):
        at = piece_span(i)
        return pltpu.make_async_copy(action_ref.at[freqs, :, at], own.at[freqs, :, at], sem)

    def own_edge(e, i):
        return own_part(pl.ds(edges[e], HALO), i, own_edge_sem.at[e, i])

    def own_inner(i):
        return own_part(pl.ds(inner, inner_size), i, own_sem.at[i])

    for i in range(PIECES):
        for e in range(len(edges)):
            own_edge(e, i).start()
    def bit(axis, amount):
        return lax.rem(lax.div(places[axis][0], amount), 2)

    neighbours = [(0, has_next, has_last, "pts")]
    if n_freq > 2:
        neighbours.append((1, has_above, has_below, "freq"))
    barrier = pltpu.get_barrier_semaphore()

    def greet(where):
        pl.semaphore_signal(barrier, inc=1, device_id=where, device_id_type=MESH)

    last_dir = n_dir - 1

    @pl.when(dir_at < last_dir)
    def _():
        greet({"dir": dir_up})

    @pl.when(dir_at == 1)
    def _():
        greet({"dir": dir_down})

    @pl.when(dir_at == 0)
    def _():
        greet({"dir": dir_down})

    parents = 1 + lax.div(dir_at, last_dir)
    for stage in stages:
        for axis, kind, amount in stage:
            if kind == "swap":
                pl.when(bit(axis, amount) == 0)(functools.partial(greet, partner(axis, kind, amount)))
                parents += bit(axis, amount)
            else:
                greet(partner(axis, kind, amount))
                parents += 1
    for _, up_there, _, axis in neighbours:
        pl.when(up_there)(functools.partial(greet, {axis: places[axis][0] + 1}))
        parents += jnp.minimum(places[axis][0], 1)

    for i in range(PIECES):
        own_inner(i).start()

    loads = [
        pltpu.make_async_copy(source, target, load_sem.at[i])
        for i, (source, target) in enumerate(
            (
                (slope_hbm, slope_ref),
                (heading_hbm, heading_ref),
                (depth_hbm, depth_ref),
                (wet_hbm, wet_ref),
                (refraction_hbm, refraction_ref),
                (shifting_hbm, shifting_ref),
                (substeps_hbm, substeps_ref),
            )
        )
    ]
    for copy in loads:
        copy.start()

    def remote(src, dst, send, recv, where):
        return pltpu.make_async_remote_copy(
            src_ref=src, dst_ref=dst, send_sem=send, recv_sem=recv, device_id=where, device_id_type=MESH
        )

    def depth_up():
        return remote(
            depth_hbm.at[:, pl.ds(points - LANES, LANES)],
            depth_in.at[0],
            depth_send.at[0],
            depth_recv.at[0],
            {"pts": pts_at + 1},
        )

    def depth_down():
        return remote(
            depth_hbm.at[:, pl.ds(0, LANES)],
            depth_in.at[1],
            depth_send.at[1],
            depth_recv.at[1],
            {"pts": pts_at - 1},
        )

    def halo_copy(way, freqs, at, send, recv):
        top = pl.ds(dir_local - HALO, HALO)
        source, target, where = (top, pl.ds(HALO, HALO), dir_up) if way == 0 else (
            pl.ds(0, HALO),
            pl.ds(0, HALO),
            dir_down,
        )
        return remote(own.at[freqs, source, at], halo.at[freqs, target, at], send, recv, {"dir": where})

    def edge_copy(way, e, i):
        return halo_copy(
            way, pl.ds(edges[e], HALO), piece_span(i), edge_send.at[way, e, i], edge_recv.at[way, e, i]
        )

    def dir_copy(way, c):
        return halo_copy(way, pl.ds(inner, inner_size), span(c), dir_send.at[way, c], dir_recv.at[way, c])

    above, below = lax.rem(freq_at + 1, n_freq), lax.rem(freq_at + n_freq - 1, n_freq)

    def rise(src, dst, send, recv):
        return remote(src, dst, send, recv, {"freq": above})

    def fall(src, dst, send, recv):
        return remote(src, dst, send, recv, {"freq": below})

    def freq_copies(i):
        at = piece_span(i)
        return (
            rise(
                ext.at[pl.ds(freq_local, HALO), :, at],
                ext.at[pl.ds(0, HALO), :, at],
                freq_send.at[0, i],
                freq_recv.at[0, i],
            ),
            fall(
                ext.at[pl.ds(HALO, HALO), :, at],
                ext.at[pl.ds(freq_local + HALO, HALO), :, at],
                freq_send.at[1, i],
                freq_recv.at[1, i],
            ),
        )

    def sh_copies():
        return (
            rise(
                shifting_hbm.at[pl.ds(freq_local - SUB, SUB)],
                shext.at[0],
                sh_send.at[0],
                sh_recv.at[0],
            ),
            fall(shifting_hbm.at[pl.ds(0, SUB)], shext.at[1], sh_send.at[1], sh_recv.at[1]),
        )

    def start_pair(pair):
        @pl.when(has_above)
        def _():
            pair[0].start()

        @pl.when(has_below)
        def _():
            pair[1].start()

    def wait_pair(pair):
        @pl.when(has_above)
        def _():
            pair[0].wait_send()
            pair[1].wait_recv()

        @pl.when(has_below)
        def _():
            pair[1].wait_send()
            pair[0].wait_recv()

    def report(sem, where):
        pl.semaphore_signal(sem, inc=1, device_id=where, device_id_type=MESH)

    pl.semaphore_wait(barrier, parents)

    @pl.when(dir_at > 1)
    def _():
        report(dir_ready, {"dir": dir_down})

    @pl.when(dir_at == last_dir)
    def _():
        report(dir_ready, {"dir": dir_up})

    for at, stage in enumerate(stages):
        for axis, kind, amount in stage:
            if kind == "swap":
                below_there = bit(axis, amount) == 1
                pl.when(below_there)(functools.partial(report, stage_ready.at[at], partner(axis, kind, amount)))
    for i, up_there, down_there, axis in neighbours:
        pl.when(down_there)(functools.partial(report, next_ready.at[i], {axis: places[axis][0] - 1}))
    def start_edges(way, low=0, high=PIECES):
        for i in range(low, high):
            for e in range(len(edges)):
                edge_copy(way, e, i).start()

    def start_inner(first, ahead):
        for c in range(ahead):
            dir_copy(first, c).start()

        @pl.loop(0, chunks - ahead)
        def _(c):
            dir_copy(first, c + ahead).start()
            dir_copy(1 - first, c).start()

        for c in range(chunks - ahead, chunks):
            dir_copy(1 - first, c).start()

    for i in range(PIECES):
        for e in range(len(edges)):
            own_edge(e, i).wait()

    is_end = (dir_at == 0) | (dir_at == last_dir)

    @pl.when(dir_at == 0)
    def _():
        start_edges(0, 0, 1)

    @pl.when(dir_at == last_dir)
    def _():
        start_edges(0, 0, 1)

    @pl.when(jnp.logical_not(is_end))
    def _():
        start_edges(1)


    @pl.when(dir_at < last_dir)
    def _():
        pl.semaphore_wait(dir_ready, 1)

    for i in range(PIECES):
        own_inner(i).wait()

    @pl.when(dir_at == 0)
    def _():
        for i in range(PIECES):
            start_edges(1, i, i + 1)
            if i + 1 < PIECES:
                start_edges(0, i + 1, i + 2)
        start_inner(1, 3)

    @pl.when(dir_at == last_dir)
    def _():
        for i in range(PIECES):
            start_edges(1, i, i + 1)
            if i + 1 < PIECES:
                start_edges(0, i + 1, i + 2)
        start_inner(0, LEAD)

    @pl.when(jnp.logical_not(is_end))
    def _():
        start_edges(0)
        start_inner(0, 0)

    for at, stage in enumerate(stages):
        for axis, kind, amount in stage:
            if kind == "swap":

                @pl.when(bit(axis, amount) == 0)
                def _():
                    pl.semaphore_wait(stage_ready.at[at], 1)

    for i, up_there, down_there, axis in neighbours:

        @pl.when(up_there)
        def _():
            pl.semaphore_wait(next_ready.at[i], 1)

    @pl.when(has_next)
    def _():
        depth_up().start()

    @pl.when(has_last)
    def _():
        depth_down().start()

    if n_freq > 1:
        start_pair(sh_copies())

    row = lax.broadcasted_iota(jnp.int32, (rows, CHUNK), 0)
    offset = jnp.where(row >= rows - HALO, row - rows, row)
    angle = ((dir_at * dir_local + offset).astype(jnp.float32) + 0.5) * (2.0 * math.pi / DIR)
    trig[0] = jnp.sin(angle)
    trig[1] = jnp.cos(angle)
    half = lax.broadcasted_iota(jnp.int32, (DIR // 2, LANES), 0)
    half_angle = (half.astype(jnp.float32) + 0.5) * (2.0 * math.pi / DIR)
    half_sin, half_cos = jnp.sin(half_angle), jnp.cos(half_angle)
    for copy in loads:
        copy.wait()
    wet = wet_ref[...].astype(jnp.float32)
    trig_row = (jnp.sin(slope_ref[...]), jnp.cos(slope_ref[...]), jnp.sin(heading_ref[...]), jnp.cos(heading_ref[...]))
    turn_row[1:2, :] = trig_row[0]
    turn_row[2:3, :] = trig_row[1]
    shift_row[1:2, :] = trig_row[2]
    shift_row[2:3, :] = trig_row[3]

    @pl.when(jnp.logical_not(has_below))
    def _():
        @pl.loop(0, HALO)
        def _(f):
            ext[f] = jnp.zeros((dir_local, points), jnp.float32)

    @pl.when(jnp.logical_not(has_above))
    def _():
        @pl.loop(freq_local + HALO, freq_local + 2 * HALO)
        def _(f):
            ext[f] = jnp.zeros((dir_local, points), jnp.float32)

    @pl.when(has_next)
    def _():
        depth_up().wait_send()
        depth_down().wait_recv()

    @pl.when(has_last)
    def _():
        depth_down().wait_send()
        depth_up().wait_recv()

    depth = depth_ref[...]
    lane = lax.broadcasted_iota(jnp.int32, (1, points), 1)
    before = jnp.where(pts_at == 0, depth[:, :1], depth_in[0][:, LANES - 1 :])
    after = jnp.where(pts_at == n_pts - 1, depth[:, points - 1 :], depth_in[1][:, :1])
    left = jnp.where(lane == 0, before, pltpu.roll(depth, 1, 1))
    right = jnp.where(lane == points - 1, after, pltpu.roll(depth, points - 1, 1))
    slope = (right - left) * 0.5 * wet
    turn_row[0:1, :] = slope
    shift_row[0:1, :] = wet

    def peak_step(i, carry):
        turn, shift = carry
        part = pl.ds(pl.multiple_of(i * LANES, LANES), LANES)
        sines = jnp.abs(half_sin * turn_row[2:3, part] - half_cos * turn_row[1:2, part])
        cosines = jnp.abs(half_cos * shift_row[2:3, part] + half_sin * shift_row[1:2, part])
        turn_peak = jnp.max(sines, axis=0, keepdims=True) * jnp.abs(turn_row[0:1, part])
        shift_peak = jnp.max(cosines, axis=0, keepdims=True) * shift_row[0:1, part]
        turn = jnp.maximum(turn, jnp.abs(refraction_ref[:, part]) * turn_peak)
        shift = jnp.maximum(shift, jnp.abs(shifting_ref[:, part]) * shift_peak)
        return turn, shift

    zero = jnp.zeros((freq_local, LANES), jnp.float32)
    turn, shift = lax.fori_loop(0, points // LANES, peak_step, (zero, zero))
    turn = jnp.max(jnp.max(turn, axis=0, keepdims=True), axis=1, keepdims=True)
    shift = jnp.max(jnp.max(shift, axis=0, keepdims=True), axis=1, keepdims=True)
    tile = lax.broadcasted_iota(jnp.int32, (SUB, LANES), 0)
    peaks[0] = jnp.where(tile < SUB // 2, turn, shift)

    def peak_copy(source, slot, move):
        return remote(
            peaks.at[source], peaks.at[slot], peak_send.at[slot], peak_recv.at[slot], partner(*move)
        )

    slots, taken = [], 1
    for stage in stages:
        slots.append((taken - 1, [(taken + i, move) for i, move in enumerate(stage)]))
        taken += len(stage) + 1
    for slot, move in slots[0][1] if slots else []:
        peak_copy(0, slot, move).start()

    for block in range(points // BLK):
        part = pl.ds(block * BLK, BLK)
        count_row[0:1, part] = jnp.broadcast_to(
            substeps_ref[0:1, block : block + 1].astype(jnp.float32), (1, BLK)
        )
    count = count_row[0:1, :]
    for k in range(1, KMAX):
        count_row[k : k + 1, :] = jnp.where(count > k, 1.0, 0.0)

    if n_freq > 1:
        wait_pair(sh_copies())
    face_rows = freq_local + 2 * HALO
    first = freq_at * freq_local - HALO

    @pl.loop(0, points // CHUNK)
    def _(c):
        part = span(c)
        window = jnp.concatenate(
            [shext[0, :, part][SUB - HALO :], shifting_ref[:, part], shext[1, :, part][:HALO]], axis=0
        )
        following = jnp.concatenate([window[1:], window[:1]], axis=0)
        mark = first + lax.broadcasted_iota(jnp.int32, (face_rows, CHUNK), 0)
        valid = (mark >= 0) & (mark + 1 <= FREQ - 1)
        face = jnp.where(valid, 0.5 * (window + following), 0.0)
        face_shift[:face_rows, :, part] = face[:, None, :]
        for k in range(1, KMAX):
            face_shift[k * face_rows : (k + 1) * face_rows, :, part] = (face * count_row[k : k + 1, part])[:, None, :]

    top = peaks[0]
    for at, (source, moves) in enumerate(slots):
        for slot, move in moves:
            if at:
                peak_copy(source, slot, move).start()
        for slot, move in moves:
            peak_copy(source, slot, move).wait()
            top = jnp.maximum(top, peaks[slot])
        if at + 1 < len(slots):
            peaks[slots[at + 1][0]] = top
    scale_turn = 0.5 / (top[0:1, 0:1] + EPSILON)
    scale_shift = 0.5 / (top[SUB // 2 : SUB // 2 + 1, 0:1] + EPSILON)
    turn_row[0:1, :] = turn_row[0:1, :] * scale_turn / count
    shift_row[3:4, :] = shift_row[0:1, :] * scale_shift / count

    def active_of(part):
        return [None] + [count_row[k : k + 1, part] for k in range(1, KMAX)]

    def turn_face(part):
        speed = (trig[0] * turn_row[2:3, part] - trig[1] * turn_row[1:2, part]) * turn_row[0:1, part]
        return 0.5 * (speed + pltpu.roll(speed, rows - 1, 0))

    def shift_speed(part):
        width = part.size
        return (
            trig[1, :dir_local, :width] * shift_row[2:3, part] + trig[0, :dir_local, :width] * shift_row[1:2, part]
        ) * shift_row[3:4, part]

    def turn_some(c, start, size):
        part = span(c)
        face = turn_face(part)
        forward = face > 0.0
        active = active_of(part)

        def one(f):
            ext[HALO + f, :, part] = turn_row_of(
                f, part, own, halo, refraction_ref, face, forward, active, rows, dir_local
            )

        @pl.loop(0, size // 2)
        def _(i):
            one(start + 2 * i)
            one(start + 2 * i + 1)

    def shift_chunk(c):
        @pl.loop(0, CHUNK // LANES)
        def _(h):
            part = pl.ds(pl.multiple_of(c * CHUNK + h * LANES, LANES), LANES)

            def store(f, value):
                out_ref[f, :, part] = value

            shift_columns(
                part,
                ext,
                lambda k, q: face_shift[k * face_rows + q, :, part],
                shift_speed(part),
                shift_row[0:1, part],
                store,
                face_rows,
            )

    per_piece = chunks // PIECES

    @pl.loop(0, PIECES)
    def _(i):
        for e in range(len(edges)):
            for way in range(2):
                edge_copy(way, e, i).wait()

        @pl.loop(0, per_piece)
        def _(c):
            for start in edges:
                turn_some(i * per_piece + c, start, HALO)

        if n_freq > 1:
            start_pair(freq_copies(i))

    @pl.loop(0, PIECES)
    def _(i):
        if n_freq > 1:
            wait_pair(freq_copies(i))

        @pl.loop(0, jnp.where(i == PIECES - 1, per_piece - 1, per_piece))
        def _(j):
            c = i * per_piece + j
            for way in range(2):
                dir_copy(way, c).wait()
            turn_some(c, inner, inner_size)
            shift_chunk(c)

    end = span(chunks - 1)
    tail_own[...] = own[:, :, end]
    tail_ext[...] = ext[:, :, end]
    tail_refraction[...] = refraction_ref[:, end]
    tail_face[...] = turn_face(end)
    tail_speed[...] = shift_speed(end)
    tail_steps[...] = face_shift[:, :, end]
    for k in range(1, KMAX):
        tail_rows[k : k + 1, :] = count_row[k : k + 1, end]
    tail_rows[0:1, :] = shift_row[0:1, end]
    for way in range(2):
        dir_copy(way, chunks - 1).wait()
    tail_halo[...] = halo[:, :, end]


def finish(
    n_freq,
    done,
    tail_own,
    tail_halo,
    tail_ext,
    tail_refraction,
    tail_face,
    tail_speed,
    tail_steps,
    tail_rows,
    out_hbm,
    ext,
    last,
    main_sem,
    last_sem,
):
    freq_local, dir_local, points = done.shape
    width = tail_own.shape[2]
    rows = tail_face.shape[0]
    pieces = main_sem.shape[0]
    each = freq_local // pieces
    head = points - width

    def main_copy(i):
        freqs = pl.ds(i * each, each)
        at = pl.ds(0, head)
        return pltpu.make_async_copy(done.at[freqs, :, at], out_hbm.at[freqs, :, at], main_sem.at[i])

    for i in range(pieces):
        main_copy(i).start()

    freq_at = lax.axis_index("freq")
    if n_freq == 1:
        inner, inner_size = 0, freq_local
    elif n_freq == 2:
        inner, inner_size = jnp.where(freq_at < n_freq - 1, 0, HALO), freq_local - HALO
    else:
        inner, inner_size = HALO, freq_local - 2 * HALO

    ext[...] = tail_ext[...]
    everything = pl.ds(0, width)
    face = tail_face[...]
    forward = face > 0.0
    active = [None] + [tail_rows[k : k + 1, :] for k in range(1, KMAX)]

    def one(f):
        ext[HALO + f] = turn_row_of(
            f, everything, tail_own, tail_halo, tail_refraction, face, forward, active, rows, dir_local
        )

    @pl.loop(0, inner_size // 2)
    def _(i):
        one(inner + 2 * i)
        one(inner + 2 * i + 1)

    @pl.loop(0, width // LANES)
    def _(h):
        part = pl.ds(pl.multiple_of(h * LANES, LANES), LANES)

        def store(f, value):
            last[f, :, part] = value

        shift_columns(
            part,
            ext,
            lambda k, q: tail_steps[k * (freq_local + 2 * HALO) + q, :, part],
            tail_speed[:, part],
            tail_rows[0:1, part],
            store,
            freq_local + 2 * HALO,
        )

    final = pltpu.make_async_copy(last, out_hbm.at[:, :, pl.ds(head, width)], last_sem)
    final.start()
    for i in range(pieces):
        main_copy(i).wait()
    final.wait()


def local(mesh, action, bathymetry, refraction, shifting, heading, slope_angle, wet_mask, substeps):
    freq_local, dir_local, points = action.shape
    n_pts, n_dir, n_freq = mesh.shape["pts"], mesh.shape["dir"], mesh.shape["freq"]
    chunks = points // CHUNK
    rows = -(-(dir_local + 2 * HALO) // SUB) * SUB
    face_rows = freq_local + 2 * HALO
    stages = peak_stages(n_pts, n_freq)
    n_slots = 1 + sum(len(stage) + 1 for stage in stages)
    vmem = pl.BlockSpec(memory_space=pltpu.VMEM)
    hbm = pl.BlockSpec(memory_space=pltpu.HBM)
    dma = pltpu.SemaphoreType.DMA
    f32 = jnp.float32
    n_edges = max(1, min(2, n_freq - 1))
    shapes = [
        (freq_local, dir_local, points),
        (freq_local, dir_local, CHUNK),
        (freq_local, 2 * HALO, CHUNK),
        (face_rows, dir_local, CHUNK),
        (freq_local, CHUNK),
        (rows, CHUNK),
        (dir_local, CHUNK),
        (KMAX * face_rows, 1, CHUNK),
        (SUB, CHUNK),
    ]
    parts = pl.pallas_call(
        functools.partial(kernel, n_pts, n_dir, n_freq),
        out_shape=[jax.ShapeDtypeStruct(shape, f32) for shape in shapes],
        in_specs=[hbm] * 8,
        out_specs=[vmem] * len(shapes),
        scratch_shapes=[
            pltpu.VMEM((freq_local, dir_local, points), f32),
            pltpu.VMEM((freq_local, 2 * HALO, points), f32),
            pltpu.VMEM((face_rows, dir_local, points), f32),
            pltpu.VMEM((2, SUB, points), f32),
            pltpu.VMEM((KMAX * face_rows, 1, points), f32),
            pltpu.VMEM((1, points), f32),
            pltpu.VMEM((freq_local, points), f32),
            pltpu.VMEM((freq_local, points), f32),
            pltpu.VMEM((1, points), f32),
            pltpu.VMEM((1, points), f32),
            pltpu.VMEM((1, points), jnp.int32),
            pltpu.VMEM((1, points // BLK), jnp.int32),
            pltpu.VMEM((SUB, points), f32),
            pltpu.VMEM((SUB, points), f32),
            pltpu.VMEM((SUB, points), f32),
            pltpu.VMEM((2, rows, CHUNK), f32),
            pltpu.VMEM((2, 1, LANES), f32),
            pltpu.VMEM((n_slots, SUB, LANES), f32),
            dma((PIECES,)),
            dma((n_edges, PIECES)),
            dma((7,)),
            dma((2, n_edges, PIECES)),
            dma((2, n_edges, PIECES)),
            dma((2, chunks)),
            dma((2, chunks)),
            dma((2, PIECES)),
            dma((2, PIECES)),
            dma((2,)),
            dma((2,)),
            dma((2,)),
            dma((2,)),
            dma((n_slots,)),
            dma((n_slots,)),
            pltpu.SemaphoreType.REGULAR,
            pltpu.SemaphoreType.REGULAR((max(1, len(stages)),)),
            pltpu.SemaphoreType.REGULAR((2,)),
        ],
        compiler_params=pltpu.CompilerParams(
            collective_id=0, has_side_effects=True, vmem_limit_bytes=44 * 1024 * 1024
        ),
    )(
        *[
            pltpu.with_memory_space_constraint(array, pltpu.HBM)
            for array in (
                action,
                bathymetry.reshape(1, points),
                refraction,
                shifting,
                heading.reshape(1, points),
                slope_angle.reshape(1, points),
                wet_mask.reshape(1, points),
                substeps.reshape(1, -1),
            )
        ]
    )
    return pl.pallas_call(
        functools.partial(finish, n_freq),
        out_shape=jax.ShapeDtypeStruct(action.shape, f32),
        in_specs=[vmem] * len(shapes),
        out_specs=hbm,
        scratch_shapes=[
            pltpu.VMEM((face_rows, dir_local, CHUNK), f32),
            pltpu.VMEM((freq_local, dir_local, CHUNK), f32),
            dma((6,)),
            dma(()),
        ],
        compiler_params=pltpu.CompilerParams(vmem_limit_bytes=8 * 1024 * 1024),
    )(*parts)


def solution(mesh):
    placed = (
        P("freq", "dir", "pts"),
        P("pts"),
        P("freq", "pts"),
        P("freq", "pts"),
        P("pts"),
        P("pts"),
        P("pts"),
        P("pts"),
    )
    return jax.shard_map(
        functools.partial(local, mesh),
        mesh=mesh,
        in_specs=placed,
        out_specs=P("freq", "dir", "pts"),
        check_vma=False,
    )
```
